32 devices in a mesh: aux: 4 (over x, core), row: 8 (over z, y).
Axes of the slice: x: 2, y: 2, z: 4, core: 2. Of those that a mesh axis runs over, the one named last changes fastest.
Arguments:
- integrals: bfloat16 [4, 8192, 8192], P('aux', 'row'), may hold values from -6 to 6
- orbitals: bfloat16 [8192, 768], P('row'), may hold values from -0.0011901855 to 0.0011901855
Outputs:
- exchange_matrix: float32 [8192, 8192], P('row', 'aux')
The draws below stay inside these ranges and needn't reach their ends.
All inputs are finite; a program needn't handle non-finite values.
Results may differ from the reference program's by a relative error of at most 0.0033.
Values may be sent and summed in bfloat16 or wider, within the bound.
A program may use at most 128 MiB of HBM per device.

```python
import jax
import jax.numpy as jnp

N = 8192
OCC = 768
NAUX = 4


def levels(stream_key, shape, pieces, smallest, largest):
    gain = 1.0
    for position, parts in pieces:
        steps = jax.random.uniform(jax.random.fold_in(jax.random.fold_in(stream_key, 6), position), (parts,), jnp.float32, smallest / len(pieces), largest / len(pieces))
        gain = gain * jnp.repeat(jnp.exp(steps), shape[position] // parts).reshape((-1,) + (1,) * (len(shape) - 1 - position))
    return gain


def normal_values(rng, dims, spread, limit, cuts=(), dtype=jnp.bfloat16):
    values = spread * jax.random.normal(rng, dims, jnp.float32)
    if cuts:
        values = values * levels(rng, dims, cuts, -0.22, 0.18)
    return jnp.clip(values, -limit, limit).astype(dtype)


def setup_inputs(seed: int = 0) -> dict:
    arg_keys = jax.random.split(jax.random.key(seed), 3)
    return {
        "integrals": normal_values(arg_keys[0], (NAUX, N, N), 1.0, 6.0, ((0, 4), (1, 8))),
        "orbitals": normal_values(arg_keys[1], (N, OCC), ((N * NAUX * OCC) ** -0.5), 0.0011901855, ((0, 8),)),
    }


def reference(integrals, orbitals):
    halves = []
    for index in range(NAUX):
        product = jnp.dot(integrals[index], orbitals, preferred_element_type=jnp.float32)
        halves.append(product.astype(jnp.bfloat16))
    joined = jnp.concatenate(halves, axis=1)
    return jnp.dot(joined, joined.T, preferred_element_type=jnp.float32)
```

```python
import functools

import jax
import jax.numpy as jnp
from jax import lax
from jax.experimental import pallas as pl
from jax.experimental.pallas import tpu as pltpu
from jax.sharding import PartitionSpec as P

MESH = pl.DeviceIdType.MESH
CHUNK = 128
TILE = 256


def kernel(aux, rows_axis, b_hbm, c_hbm, out_hbm, b, c, h, k_acc, h_acc, *sems):
    (local_b, local_c, cz_s, cz_r, cy_s, cy_r, cx_s, cx_r,
     hx_s, hx_r, hz_s, hz_r, hy_s, hy_r, out_sem) = sems
    span = rows_axis // aux
    chunks, _, n_rows, width = c.shape
    share = n_rows // aux
    p = lax.axis_index("aux")
    r = lax.axis_index("row")
    layer = lax.div(r, span)
    member = lax.rem(r, span)
    bits = []
    bit = aux // 2
    while bit:
        bits.append(bit)
        bit //= 2

    def row_of(at_layer, at_member):
        return at_layer * span + at_member

    next_member = row_of(layer, lax.rem(member + 1, span))
    last_member = row_of(layer, lax.rem(member + span - 1, span))
    owner = layer == p
    own_slot = jnp.where(owner, 0, 1 + member)

    def to_row(row):
        return {"device_id": {"row": row}, "device_id_type": MESH}

    def to_aux(index):
        return {"device_id": {"aux": index}, "device_id_type": MESH}

    def lower(k):
        low = k & -k if k else aux
        return [bit for bit in bits if bit < low]

    def c_piece(j, row):
        return c.at[j, row, pl.ds(pl.multiple_of(p * share, share), share)]

    def c_line(j, at_layer, way):
        piece = c_piece(j, row_of(at_layer, member))
        return pltpu.make_async_remote_copy(
            piece, piece, cz_s.at[way, j, at_layer], cz_r.at[j, at_layer],
            **to_row(row_of(layer + 2 * way - 1, member)))

    def c_member(j, at_layer, step):
        line = lax.rem(member + span - step, span)
        piece = c_piece(j, row_of(at_layer, line))
        return pltpu.make_async_remote_copy(
            piece, piece, cy_s.at[j, step, at_layer], cy_r.at[j, step, at_layer], **to_row(next_member))

    def c_aux(j, k, bit):
        source = jnp.bitwise_xor(p, k)
        piece = c.at[j, :, pl.ds(pl.multiple_of(source * share, share), share)]
        return pltpu.make_async_remote_copy(
            piece, piece, cx_s.at[j, k ^ bit], cx_r.at[j, k ^ bit], **to_aux(jnp.bitwise_xor(p, bit)))

    def lanes(k):
        return pl.ds(k * width, width)

    def h_aux(j, k, bit):
        return pltpu.make_async_remote_copy(
            h.at[0, j, :, lanes(k)], h.at[0, j, :, lanes(k ^ bit)], hx_s.at[j, k ^ bit], hx_r.at[j, k ^ bit],
            **to_aux(jnp.bitwise_xor(p, bit)))

    def h_line(j, k, way):
        return pltpu.make_async_remote_copy(
            h.at[own_slot, j, :, lanes(k)], h.at[1 + member, j, :, lanes(k)], hz_s.at[way, j, k], hz_r.at[j, k],
            **to_row(row_of(layer + 2 * way - 1, member)))

    def h_member(j, k, step):
        line = lax.rem(member + span - step, span)
        slot = own_slot if step == 0 else 1 + line
        return pltpu.make_async_remote_copy(
            h.at[slot, j, :, lanes(k)], h.at[1 + line, j, :, lanes(k)], hy_s.at[j, step, k], hy_r.at[j, step, k],
            **to_row(next_member))

    up, down = layer + 1 < aux, layer > 0

    barrier = pltpu.get_barrier_semaphore()
    for bit in bits:
        pl.semaphore_signal(barrier, 1, **to_aux(jnp.bitwise_xor(p, bit)))
    pl.semaphore_signal(barrier, 1, **to_row(next_member))
    pl.semaphore_signal(barrier, 1, **to_row(last_member))

    @pl.when(up)
    def _():
        pl.semaphore_signal(barrier, 1, **to_row(row_of(layer + 1, member)))

    @pl.when(down)
    def _():
        pl.semaphore_signal(barrier, 1, **to_row(row_of(layer - 1, member)))

    def own_c(j):
        return pltpu.make_async_copy(
            c_hbm.at[pl.ds(pl.multiple_of(p * share, share), share), pl.ds(pl.multiple_of(j * width, width), width)],
            c_piece(j, r), local_c.at[j])

    for j in range(chunks):
        own_c(j).start()
    load_b = pltpu.make_async_copy(b_hbm, b, local_b)
    load_b.start()
    pl.semaphore_wait(barrier, len(bits) + 2 + up.astype(jnp.int32) + down.astype(jnp.int32))

    def loop(count, body):
        def step(i, carry):
            body(i)
            return carry
        lax.fori_loop(0, count, step, 0)

    def pass_c(j, at_layer):
        c_member(j, at_layer, 0).start()

    def start_c(j):
        own_c(j).wait()

        @pl.when(up)
        def _():
            c_line(j, layer, 1).start()

        @pl.when(down)
        def _():
            c_line(j, layer, 0).start()

        pass_c(j, layer)

    def relay_c(j):
        for step in range(1, aux):
            @pl.when(layer - step >= 0)
            def _():
                c_line(j, layer - step, 1).wait_recv()

                @pl.when(up)
                def _():
                    c_line(j, layer - step, 1).start()

                pass_c(j, layer - step)

            @pl.when(layer + step < aux)
            def _():
                c_line(j, layer + step, 0).wait_recv()

                @pl.when(down)
                def _():
                    c_line(j, layer + step, 0).start()

                pass_c(j, layer + step)

    def spread_c(j):
        for step in range(span - 1):
            for at_layer in range(aux):
                c_member(j, at_layer, step).wait_recv()
                if step + 1 < span - 1:
                    c_member(j, at_layer, step + 1).start()
        for bit in bits:
            c_aux(j, 0, bit).start()

    def finish_c(j):
        for k in sorted(range(1, aux), key=lambda k: -(k & -k)):
            c_aux(j, k ^ (k & -k), k & -k).wait_recv()
            for bit in lower(k):
                c_aux(j, k, bit).start()

    def transform(j):
        finish_c(j)

        def block(i):
            part = jnp.dot(
                b[:, pl.ds(pl.multiple_of(i * n_rows, n_rows), n_rows)], c[j, i], preferred_element_type=jnp.float32)

            @pl.when(i == 0)
            def _():
                h_acc[...] = part

            @pl.when(i > 0)
            def _():
                h_acc[...] += part

        loop(rows_axis, block)
        h[0, j, :, lanes(0)] = h_acc[...].astype(h.dtype)
        for bit in bits:
            h_aux(j, 0, bit).start()

    def send_h(j, k):
        @pl.when(owner)
        def _():
            @pl.when(up)
            def _():
                h_line(j, k, 1).start()

            @pl.when(down)
            def _():
                h_line(j, k, 0).start()

            h_member(j, k, 0).start()

    def take_h(j, k):
        h_aux(j, k ^ (k & -k), k & -k).wait_recv()
        for bit in lower(k):
            h_aux(j, k, bit).start()
        send_h(j, k)

    def send_first(j):
        send_h(j, 0)
        for k in range(1, aux // 2):
            take_h(j, k)

    def send_rest(j):
        for k in range(aux // 2, aux):
            take_h(j, k)

    def relay_h(j, k):
        @pl.when(layer > p)
        def _():
            h_line(j, k, 1).wait_recv()

            @pl.when(up)
            def _():
                h_line(j, k, 1).start()

            h_member(j, k, 0).start()

        @pl.when(layer < p)
        def _():
            h_line(j, k, 0).wait_recv()

            @pl.when(down)
            def _():
                h_line(j, k, 0).start()

            h_member(j, k, 0).start()

    tile = min(TILE, n_rows)
    tiles = n_rows // tile

    def out_copy(n):
        columns = pl.ds(pl.multiple_of(n * tile, tile), tile)
        return pltpu.make_async_copy(k_acc.at[:, columns], out_hbm.at[:, columns], out_sem.at[n])

    def update(j, is_last):
        for step in range(span - 1):
            for k in range(aux):
                h_member(j, k, step).wait_recv()
                if step + 1 < span - 1:
                    h_member(j, k, step + 1).start()

        def block(n):
            line = lax.div(n, tiles)
            slot = jnp.where(line == member, own_slot, 1 + line)
            at = pl.ds(pl.multiple_of(lax.rem(n, tiles) * tile, tile), tile)
            part = lax.dot_general(
                h[0, j], h[slot, j, at], (((1,), (1,)), ((), ())), preferred_element_type=jnp.float32)
            columns = pl.ds(pl.multiple_of(n * tile, tile), tile)
            k_acc[:, columns] += part
            if is_last:
                out_copy(n).start()

        loop(span * tiles, block)

    loop(chunks, start_c)

    def clear(n):
        columns = pl.ds(pl.multiple_of(n * tile, tile), tile)
        k_acc[:, columns] = jnp.zeros((n_rows, tile), jnp.float32)

    loop(span * tiles, clear)

    relay_c(0)
    relay_c(1)
    spread_c(0)
    relay_c(2)
    spread_c(1)
    loop(chunks - 3, lambda i: relay_c(i + 3))
    load_b.wait()
    transform(0)
    send_first(0)
    spread_c(2)
    transform(1)
    send_rest(0)
    send_first(1)
    spread_c(3)

    def main(j):
        half = aux // 2
        for k in range(half):
            relay_h(j, k)

        @pl.when(j + 2 < chunks)
        def _():
            transform(j + 2)

        @pl.when(j + 1 < chunks)
        def _():
            send_rest(j + 1)

        @pl.when(j + 2 < chunks)
        def _():
            send_first(j + 2)

        @pl.when(j + 4 < chunks)
        def _():
            spread_c(j + 4)

        for k in range(half, aux):
            relay_h(j, k)

        @pl.when(j > 0)
        def _():
            update(j - 1, False)

    loop(chunks, main)
    update(chunks - 1, True)

    def drain(j):
        for at_layer in range(aux):
            @pl.when(jnp.logical_and(up, at_layer <= layer))
            def _():
                c_line(j, at_layer, 1).wait_send()

            @pl.when(jnp.logical_and(down, at_layer >= layer))
            def _():
                c_line(j, at_layer, 0).wait_send()

            for step in range(span - 1):
                c_member(j, at_layer, step).wait_send()
        for k in range(1, aux):
            low = k & -k
            c_aux(j, k ^ low, low).wait_send()
            h_aux(j, k ^ low, low).wait_send()
        for k in range(aux):
            @pl.when(jnp.logical_and(up, layer >= p))
            def _():
                h_line(j, k, 1).wait_send()

            @pl.when(jnp.logical_and(down, layer <= p))
            def _():
                h_line(j, k, 0).wait_send()

            for step in range(span - 1):
                h_member(j, k, step).wait_send()

    loop(chunks, drain)
    loop(span * tiles, lambda n: out_copy(n).wait())


def body(aux, rows_axis, integrals, orbitals):
    _, n_rows, n = integrals.shape
    occ = orbitals.shape[1]
    span = rows_axis // aux
    width = CHUNK
    chunks = occ // width
    dma = pltpu.SemaphoreType.DMA
    tiles = span * (n_rows // min(TILE, n_rows))
    steps = max(span - 1, 1)
    return pl.pallas_call(
        functools.partial(kernel, aux, rows_axis),
        out_shape=jax.ShapeDtypeStruct((n_rows, span * n_rows), jnp.float32),
        in_specs=[pl.BlockSpec(memory_space=pl.ANY)] * 2,
        out_specs=pl.BlockSpec(memory_space=pl.ANY),
        scratch_shapes=[
            pltpu.VMEM((n_rows, n), integrals.dtype),
            pltpu.VMEM((chunks, rows_axis, n_rows, width), orbitals.dtype),
            pltpu.VMEM((1 + span, chunks, n_rows, aux * width), jnp.bfloat16),
            pltpu.VMEM((n_rows, span * n_rows), jnp.float32),
            pltpu.VMEM((n_rows, width), jnp.float32),
            dma, dma((chunks,)),
            dma((2, chunks, aux)), dma((chunks, aux)),
            dma((chunks, steps, aux)), dma((chunks, steps, aux)),
            dma((chunks, aux)), dma((chunks, aux)),
            dma((chunks, aux)), dma((chunks, aux)),
            dma((2, chunks, aux)), dma((chunks, aux)),
            dma((chunks, steps, aux)), dma((chunks, steps, aux)),
            dma((tiles,)),
        ],
        compiler_params=pltpu.CompilerParams(
            collective_id=0, has_side_effects=True, vmem_limit_bytes=67_043_328),
    )(integrals.reshape(n_rows, n), orbitals)


def solution(mesh):
    aux, rows_axis = mesh.shape["aux"], mesh.shape["row"]
    return jax.shard_map(
        functools.partial(body, aux, rows_axis), mesh=mesh,
        in_specs=(P("aux", "row", None), P("row", None)), out_specs=P("row", "aux"), check_vma=False)
```

```python
import functools

import jax
import jax.numpy as jnp
from jax import lax
from jax.experimental import pallas as pl
from jax.experimental.pallas import tpu as pltpu
from jax.sharding import PartitionSpec as P

MESH = pl.DeviceIdType.MESH
CHUNK = 128
TILE = 256
PARTS = 4


def kernel(aux, rows_axis, b_hbm, c_hbm, out_hbm, b, c, h, k_acc, h_acc, *sems):
    (local_b, local_c, cz_s, cz_r, cy_s, cy_r, cx_s, cx_r,
     hx_s, hx_r, hz_s, hz_r, hy_s, hy_r, out_sem) = sems
    span = rows_axis // aux
    chunks, _, n_rows, width = c.shape
    share = n_rows // aux
    p = lax.axis_index("aux")
    r = lax.axis_index("row")
    layer = lax.div(r, span)
    member = lax.rem(r, span)
    bits = []
    bit = aux // 2
    while bit:
        bits.append(bit)
        bit //= 2

    def row_of(at_layer, at_member):
        return at_layer * span + at_member

    next_member = row_of(layer, lax.rem(member + 1, span))
    last_member = row_of(layer, lax.rem(member + span - 1, span))
    owner = layer == p
    own_slot = jnp.where(owner, 0, 1 + member)

    def to_row(row):
        return {"device_id": {"row": row}, "device_id_type": MESH}

    def to_aux(index):
        return {"device_id": {"aux": index}, "device_id_type": MESH}

    def lower(k):
        low = k & -k if k else aux
        return [bit for bit in bits if bit < low]

    def c_piece(j, row):
        return c.at[j, row, pl.ds(pl.multiple_of(p * share, share), share)]

    def c_line(j, at_layer, way):
        piece = c_piece(j, row_of(at_layer, member))
        return pltpu.make_async_remote_copy(
            piece, piece, cz_s.at[way, j, at_layer], cz_r.at[j, at_layer],
            **to_row(row_of(layer + 2 * way - 1, member)))

    def c_member(j, at_layer, step):
        line = lax.rem(member + span - step, span)
        piece = c_piece(j, row_of(at_layer, line))
        return pltpu.make_async_remote_copy(
            piece, piece, cy_s.at[j, step, at_layer], cy_r.at[j, step, at_layer], **to_row(next_member))

    def c_aux(j, k, bit):
        source = jnp.bitwise_xor(p, k)
        piece = c.at[j, :, pl.ds(pl.multiple_of(source * share, share), share)]
        return pltpu.make_async_remote_copy(
            piece, piece, cx_s.at[j, k ^ bit], cx_r.at[j, k ^ bit], **to_aux(jnp.bitwise_xor(p, bit)))

    def lanes(k):
        return pl.ds(k * width, width)

    def h_aux(j, k, bit):
        return pltpu.make_async_remote_copy(
            h.at[0, j, :, lanes(k)], h.at[0, j, :, lanes(k ^ bit)], hx_s.at[j, k ^ bit], hx_r.at[j, k ^ bit],
            **to_aux(jnp.bitwise_xor(p, bit)))

    part = n_rows // PARTS

    def message(slot, j, i):
        rows = pl.ds(pl.multiple_of(lax.rem(i, PARTS) * part, part), part)
        return h.at[slot, j, rows, pl.ds(pl.multiple_of(lax.div(i, PARTS) * width, width), width)]

    def h_line(j, i, way):
        return pltpu.make_async_remote_copy(
            message(own_slot, j, i), message(1 + member, j, i), hz_s.at[way, j], hz_r.at[j, i],
            **to_row(row_of(layer + 2 * way - 1, member)))

    def h_line_sent(j, way):
        return pltpu.make_async_remote_copy(
            h.at[0, j], h.at[0, j], hz_s.at[way, j], hz_r.at[j, 0], **to_row(row_of(layer + 2 * way - 1, member)))

    def h_member(j, i, step):
        line = lax.rem(member + span - step, span)
        slot = own_slot if step == 0 else 1 + line
        return pltpu.make_async_remote_copy(
            message(slot, j, i), message(1 + line, j, i), hy_s.at[j, step], hy_r.at[j, step, i],
            **to_row(next_member))

    def h_member_sent(j, step):
        return pltpu.make_async_remote_copy(
            h.at[0, j], h.at[0, j], hy_s.at[j, step], hy_r.at[j, step, 0], **to_row(next_member))

    up, down = layer + 1 < aux, layer > 0

    barrier = pltpu.get_barrier_semaphore()
    for bit in bits:
        pl.semaphore_signal(barrier, 1, **to_aux(jnp.bitwise_xor(p, bit)))
    pl.semaphore_signal(barrier, 1, **to_row(next_member))
    pl.semaphore_signal(barrier, 1, **to_row(last_member))

    @pl.when(up)
    def _():
        pl.semaphore_signal(barrier, 1, **to_row(row_of(layer + 1, member)))

    @pl.when(down)
    def _():
        pl.semaphore_signal(barrier, 1, **to_row(row_of(layer - 1, member)))

    def own_c(j):
        return pltpu.make_async_copy(
            c_hbm.at[pl.ds(pl.multiple_of(p * share, share), share), pl.ds(pl.multiple_of(j * width, width), width)],
            c_piece(j, r), local_c.at[j])

    for j in range(chunks):
        own_c(j).start()
    load_b = pltpu.make_async_copy(b_hbm, b, local_b)
    load_b.start()
    pl.semaphore_wait(barrier, len(bits) + 2 + up.astype(jnp.int32) + down.astype(jnp.int32))

    def loop_from(first, last, body):
        def step(i, carry):
            body(i)
            return carry
        lax.fori_loop(first, last, step, 0)

    def loop(count, body):
        loop_from(0, count, body)

    def pass_c(j, at_layer):
        c_member(j, at_layer, 0).start()

    def start_c(j):
        own_c(j).wait()

        @pl.when(up)
        def _():
            c_line(j, layer, 1).start()

        @pl.when(down)
        def _():
            c_line(j, layer, 0).start()

        pass_c(j, layer)

    def relay_c(j):
        for step in range(1, aux):
            @pl.when(layer - step >= 0)
            def _():
                c_line(j, layer - step, 1).wait_recv()

                @pl.when(up)
                def _():
                    c_line(j, layer - step, 1).start()

                pass_c(j, layer - step)

            @pl.when(layer + step < aux)
            def _():
                c_line(j, layer + step, 0).wait_recv()

                @pl.when(down)
                def _():
                    c_line(j, layer + step, 0).start()

                pass_c(j, layer + step)

    def spread_c(j):
        for step in range(span - 1):
            for at_layer in range(aux):
                c_member(j, at_layer, step).wait_recv()
                if step + 1 < span - 1:
                    c_member(j, at_layer, step + 1).start()
        for bit in bits:
            c_aux(j, 0, bit).start()

    def finish_c(j):
        for k in sorted(range(1, aux), key=lambda k: -(k & -k)):
            c_aux(j, k ^ (k & -k), k & -k).wait_recv()
            for bit in lower(k):
                c_aux(j, k, bit).start()

    slots = aux * PARTS
    pieces = slots // 2

    def transform(j, piece):
        @pl.when(piece == 0)
        def _():
            finish_c(j)
            h_acc[...] = jnp.zeros_like(h_acc)

        def block(i):
            h_acc[...] += jnp.dot(
                b[:, pl.ds(pl.multiple_of(i * n_rows, n_rows), n_rows)], c[j, i], preferred_element_type=jnp.float32)

        loop_from(lax.div(piece * rows_axis, pieces), lax.div((piece + 1) * rows_axis, pieces), block)

        @pl.when(piece == pieces - 1)
        def _():
            h[0, j, :, lanes(0)] = h_acc[...].astype(h.dtype)
            for bit in bits:
                h_aux(j, 0, bit).start()

            @pl.when(j > 0)
            def _():
                send_rest(j - 1)

            send_first(j)

            @pl.when(j + 2 < chunks)
            def _():
                spread_c(j + 2)

    def send_h(j, k):
        @pl.when(owner)
        def _():
            def send(i):
                @pl.when(up)
                def _():
                    h_line(j, i, 1).start()

                @pl.when(down)
                def _():
                    h_line(j, i, 0).start()

                h_member(j, i, 0).start()

            loop_from(k * PARTS, (k + 1) * PARTS, send)

    def take_h(j, k):
        h_aux(j, k ^ (k & -k), k & -k).wait_recv()
        for bit in lower(k):
            h_aux(j, k, bit).start()
        send_h(j, k)

    def send_first(j):
        send_h(j, 0)
        for k in range(1, aux // 2):
            take_h(j, k)

    def send_rest(j):
        for k in range(aux // 2, aux):
            take_h(j, k)

    def relay_h(j, i):
        @pl.when(layer > p)
        def _():
            h_line(j, i, 1).wait_recv()

            @pl.when(up)
            def _():
                h_line(j, i, 1).start()

            h_member(j, i, 0).start()

        @pl.when(layer < p)
        def _():
            h_line(j, i, 0).wait_recv()

            @pl.when(down)
            def _():
                h_line(j, i, 0).start()

            h_member(j, i, 0).start()

    tile = min(TILE, n_rows)
    tiles = n_rows // tile
    all_tiles = span * tiles

    def out_copy(n):
        columns = pl.ds(pl.multiple_of(n * tile, tile), tile)
        return pltpu.make_async_copy(k_acc.at[:, columns], out_hbm.at[:, columns], out_sem.at[n])

    def take_members(j, first, last):
        for step in range(span - 1):
            def take(i):
                h_member(j, i, step).wait_recv()
                if step + 1 < span - 1:
                    h_member(j, i, step + 1).start()
            loop_from(first, last, take)

    def add_tile(j, n, first, last):
        line = lax.div(n, tiles)
        slot = jnp.where(line == member, own_slot, 1 + line)
        at = pl.ds(pl.multiple_of(lax.rem(n, tiles) * tile, tile), tile)
        some = pl.ds(first * width, (last - first) * width)
        k_acc[:, pl.ds(pl.multiple_of(n * tile, tile), tile)] += lax.dot_general(
            h[0, j, :, some], h[slot, j, at, some], (((1,), (1,)), ((), ())), preferred_element_type=jnp.float32)

    def update(j, piece, count):
        @pl.when(piece == 0)
        def _():
            take_members(j, 0, slots)

        loop_from(lax.div(piece * all_tiles, count), lax.div((piece + 1) * all_tiles, count),
                  lambda n: add_tile(j, n, 0, aux))

    def last_update(j):
        take_members(j, 0, slots - PARTS)
        loop(all_tiles, lambda n: add_tile(j, n, 0, aux - 1))
        take_members(j, slots - PARTS, slots)

        def finish(n):
            add_tile(j, n, aux - 1, aux)
            out_copy(n).start()

        loop(all_tiles, finish)

    loop(chunks, start_c)

    def clear(n):
        columns = pl.ds(pl.multiple_of(n * tile, tile), tile)
        k_acc[:, columns] = jnp.zeros((n_rows, tile), jnp.float32)

    loop(span * tiles, clear)

    relay_c(0)
    relay_c(1)
    spread_c(0)
    relay_c(2)
    spread_c(1)
    loop(chunks - 3, lambda i: relay_c(i + 3))
    load_b.wait()
    loop(pieces, lambda piece: transform(0, piece))

    quarter = slots // 4

    def main(j):
        def slot(i):
            relay_h(j, i)
            early = jnp.logical_and(j == 1, i < quarter)
            chunk = jnp.where(j == 0, jnp.where(i < pieces, 1, 2), jnp.where(early, 2, j + 2))
            piece = jnp.where(
                j == 0, jnp.where(i < pieces, i, i - 3 * quarter), jnp.where(early, i + quarter, i - quarter))
            now = jnp.logical_and(jnp.logical_and(piece >= 0, piece < pieces), chunk < chunks)

            @pl.when(now)
            def _():
                transform(chunk, piece)

            @pl.when(jnp.logical_and(j > 0, i >= 3 * quarter))
            def _():
                update(j - 1, i - 3 * quarter, quarter)

        loop(slots, slot)

        @pl.when(j == max(chunks - 2, 0))
        def _():
            send_rest(chunks - 1)

    loop(chunks, main)
    last_update(chunks - 1)

    def drain(j):
        for at_layer in range(aux):
            @pl.when(jnp.logical_and(up, at_layer <= layer))
            def _():
                c_line(j, at_layer, 1).wait_send()

            @pl.when(jnp.logical_and(down, at_layer >= layer))
            def _():
                c_line(j, at_layer, 0).wait_send()

            for step in range(span - 1):
                c_member(j, at_layer, step).wait_send()
        for k in range(1, aux):
            low = k & -k
            c_aux(j, k ^ low, low).wait_send()
            h_aux(j, k ^ low, low).wait_send()

        @pl.when(jnp.logical_and(up, layer >= p))
        def _():
            h_line_sent(j, 1).wait_send()

        @pl.when(jnp.logical_and(down, layer <= p))
        def _():
            h_line_sent(j, 0).wait_send()

        for step in range(span - 1):
            h_member_sent(j, step).wait_send()

    loop(chunks, drain)
    loop(all_tiles, lambda n: out_copy(n).wait())


def body(aux, rows_axis, integrals, orbitals):
    _, n_rows, n = integrals.shape
    occ = orbitals.shape[1]
    span = rows_axis // aux
    width = CHUNK
    chunks = occ // width
    dma = pltpu.SemaphoreType.DMA
    tiles = span * (n_rows // min(TILE, n_rows))
    steps = max(span - 1, 1)
    return pl.pallas_call(
        functools.partial(kernel, aux, rows_axis),
        out_shape=jax.ShapeDtypeStruct((n_rows, span * n_rows), jnp.float32),
        in_specs=[pl.BlockSpec(memory_space=pl.ANY)] * 2,
        out_specs=pl.BlockSpec(memory_space=pl.ANY),
        scratch_shapes=[
            pltpu.VMEM((n_rows, n), integrals.dtype),
            pltpu.VMEM((chunks, rows_axis, n_rows, width), orbitals.dtype),
            pltpu.VMEM((1 + span, chunks, n_rows, aux * width), jnp.bfloat16),
            pltpu.VMEM((n_rows, span * n_rows), jnp.float32),
            pltpu.VMEM((n_rows, width), jnp.float32),
            dma, dma((chunks,)),
            dma((2, chunks, aux)), dma((chunks, aux)),
            dma((chunks, steps, aux)), dma((chunks, steps, aux)),
            dma((chunks, aux)), dma((chunks, aux)),
            dma((chunks, aux)), dma((chunks, aux)),
            dma((2, chunks)), dma((chunks, aux * PARTS)),
            dma((chunks, steps)), dma((chunks, steps, aux * PARTS)),
            dma((tiles,)),
        ],
        compiler_params=pltpu.CompilerParams(
            collective_id=0, has_side_effects=True, vmem_limit_bytes=67_043_328),
    )(integrals.reshape(n_rows, n), orbitals)


def solution(mesh):
    aux, rows_axis = mesh.shape["aux"], mesh.shape["row"]
    return jax.shard_map(
        functools.partial(body, aux, rows_axis), mesh=mesh,
        in_specs=(P("aux", "row", None), P("row", None)), out_specs=P("row", "aux"), check_vma=False)
```

```python
import functools

import jax
import jax.numpy as jnp
from jax import lax
from jax.experimental import pallas as pl
from jax.experimental.pallas import tpu as pltpu
from jax.sharding import PartitionSpec as P

MESH = pl.DeviceIdType.MESH
CHUNK = 128
TILE = 256
PARTS = 4
TRANSIT = 6


def kernel(aux, rows_axis, b_hbm, c_hbm, k_acc, b, c, h, t, h_acc, *sems):
    (local_b, local_c, cz_s, cz_r, cy_s, cy_r, cx_s, cx_r,
     hx_s, hx_r, hz_s, hz_r, hy_s, hy_r, ty_s, tz_s, tx_s, t_r) = sems
    span = rows_axis // aux
    chunks, _, n_rows, width = c.shape
    share = n_rows // aux
    p = lax.axis_index("aux")
    r = lax.axis_index("row")
    layer = lax.div(r, span)
    member = lax.rem(r, span)
    bits = []
    bit = aux // 2
    while bit:
        bits.append(bit)
        bit //= 2

    def row_of(at_layer, at_member):
        return at_layer * span + at_member

    next_member = row_of(layer, lax.rem(member + 1, span))
    last_member = row_of(layer, lax.rem(member + span - 1, span))
    owner = layer == p
    own_slot = jnp.where(owner, 0, 1 + member)

    half = aux // 2
    partner = jnp.bitwise_xor(p, half)
    first_transit, first_own = half * PARTS, (half + 1) * PARTS
    last_transit = first_transit + TRANSIT

    def ahead(index):
        return jnp.where(index < half, layer - index, index - layer)

    main_far, transit_far = ahead(p), ahead(partner)
    main_up, transit_way = p < half, jnp.where(partner < half, 1, 0)
    transit_row = row_of(layer + 2 * transit_way - 1, member)
    transit_on = jnp.logical_and(transit_far >= 0, jnp.where(partner < half, layer + 1 < aux, layer > 0))

    def own_by_transit(i):
        return jnp.logical_and(i >= first_own, i < last_transit)

    def other_by_transit(i):
        return jnp.logical_and(main_far >= 0, jnp.logical_and(i >= first_transit, i < first_own))

    def to_row(row):
        return {"device_id": {"row": row}, "device_id_type": MESH}

    def to_aux(index):
        return {"device_id": {"aux": index}, "device_id_type": MESH}

    def lower(k):
        low = k & -k if k else aux
        return [bit for bit in bits if bit < low]

    def c_piece(j, row):
        return c.at[j, row, pl.ds(pl.multiple_of(p * share, share), share)]

    def c_line(j, at_layer, way):
        piece = c_piece(j, row_of(at_layer, member))
        return pltpu.make_async_remote_copy(
            piece, piece, cz_s.at[way, j, at_layer], cz_r.at[j, at_layer],
            **to_row(row_of(layer + 2 * way - 1, member)))

    def c_member(j, at_layer, step):
        line = lax.rem(member + span - step, span)
        piece = c_piece(j, row_of(at_layer, line))
        return pltpu.make_async_remote_copy(
            piece, piece, cy_s.at[j, step, at_layer], cy_r.at[j, step, at_layer], **to_row(next_member))

    def c_aux(j, k, bit):
        source = jnp.bitwise_xor(p, k)
        piece = c.at[j, :, pl.ds(pl.multiple_of(source * share, share), share)]
        return pltpu.make_async_remote_copy(
            piece, piece, cx_s.at[j, k ^ bit], cx_r.at[j, k ^ bit], **to_aux(jnp.bitwise_xor(p, bit)))

    def lanes(k):
        return pl.ds(k * width, width)

    def h_aux(j, k, bit):
        return pltpu.make_async_remote_copy(
            h.at[0, j, :, lanes(k)], h.at[0, j, :, lanes(k ^ bit)], hx_s.at[j, k ^ bit], hx_r.at[j, k ^ bit],
            **to_aux(jnp.bitwise_xor(p, bit)))

    part = n_rows // PARTS
    slots = aux * PARTS
    pieces = slots // 2

    def message(slot, j, i):
        rows = pl.ds(pl.multiple_of(lax.rem(i, PARTS) * part, part), part)
        return h.at[slot, j, rows, pl.ds(pl.multiple_of(lax.div(i, PARTS) * width, width), width)]

    def h_line(j, i, way):
        return pltpu.make_async_remote_copy(
            message(own_slot, j, i), message(1 + member, j, i), hz_s.at[way, j], hz_r.at[j, i],
            **to_row(row_of(layer + 2 * way - 1, member)))

    def messages(j, count):
        return h.at[0, j, pl.ds(0, n_rows * count // slots)]

    def h_line_sent(j, way, count):
        return pltpu.make_async_remote_copy(
            messages(j, count), messages(j, count), hz_s.at[way, j], hz_r.at[j, 0], **to_row(row_of(layer + 2 * way - 1, member)))

    def h_member(j, i, step):
        line = lax.rem(member + span - step, span)
        slot = own_slot if step == 0 else 1 + line
        return pltpu.make_async_remote_copy(
            message(slot, j, i), message(1 + line, j, i), hy_s.at[j, step], hy_r.at[j, step, i],
            **to_row(next_member))

    def h_member_sent(j, step, count):
        return pltpu.make_async_remote_copy(
            messages(j, count), messages(j, count), hy_s.at[j, step], hy_r.at[j, step, 0], **to_row(next_member))

    def t_member(j, i):
        return pltpu.make_async_remote_copy(
            message(0, j, i), t.at[j, i], ty_s.at[j], t_r.at[j, i], **to_row(next_member))

    def t_line(source, j, i):
        return pltpu.make_async_remote_copy(source, t.at[j, i], tz_s.at[j], t_r.at[j, i], **to_row(transit_row))

    def t_other(j, i):
        at = first_transit + i
        return pltpu.make_async_remote_copy(
            t.at[j, i], message(1 + lax.rem(member + span - 1, span), j, at), tx_s.at[j], hy_r.at[j, 0, at],
            **to_aux(partner))

    def t_own(j, i):
        at = first_transit + i
        return pltpu.make_async_remote_copy(
            t.at[j, i], message(1 + member, j, at), tx_s.at[j], hz_r.at[j, at], **to_aux(partner))

    def t_sent(j, count, sem, where):
        some = t.at[j, pl.ds(0, count)]
        return pltpu.make_async_remote_copy(some, some, sem.at[j], t_r.at[j, 0], **where)

    up, down = layer + 1 < aux, layer > 0

    barrier = pltpu.get_barrier_semaphore()
    for bit in bits:
        pl.semaphore_signal(barrier, 1, **to_aux(jnp.bitwise_xor(p, bit)))
    pl.semaphore_signal(barrier, 1, **to_row(next_member))
    pl.semaphore_signal(barrier, 1, **to_row(last_member))

    @pl.when(up)
    def _():
        pl.semaphore_signal(barrier, 1, **to_row(row_of(layer + 1, member)))

    @pl.when(down)
    def _():
        pl.semaphore_signal(barrier, 1, **to_row(row_of(layer - 1, member)))

    def own_c(j):
        return pltpu.make_async_copy(
            c_hbm.at[pl.ds(pl.multiple_of(p * share, share), share), pl.ds(pl.multiple_of(j * width, width), width)],
            c_piece(j, r), local_c.at[j])

    for j in range(chunks):
        own_c(j).start()
    load_b = pltpu.make_async_copy(b_hbm, b, local_b)
    load_b.start()
    pl.semaphore_wait(barrier, len(bits) + 2 + up.astype(jnp.int32) + down.astype(jnp.int32))

    def loop_from(first, last, body):
        def step(i, carry):
            body(i)
            return carry
        lax.fori_loop(first, last, step, 0)

    def loop(count, body):
        loop_from(0, count, body)

    def pass_c(j, at_layer):
        c_member(j, at_layer, 0).start()

    def start_c(j):
        own_c(j).wait()

        @pl.when(up)
        def _():
            c_line(j, layer, 1).start()

        @pl.when(down)
        def _():
            c_line(j, layer, 0).start()

        pass_c(j, layer)

    def relay_c(j):
        for step in range(1, aux):
            @pl.when(layer - step >= 0)
            def _():
                c_line(j, layer - step, 1).wait_recv()

                @pl.when(up)
                def _():
                    c_line(j, layer - step, 1).start()

                pass_c(j, layer - step)

            @pl.when(layer + step < aux)
            def _():
                c_line(j, layer + step, 0).wait_recv()

                @pl.when(down)
                def _():
                    c_line(j, layer + step, 0).start()

                pass_c(j, layer + step)

    def spread_c(j):
        for step in range(span - 1):
            for at_layer in range(aux):
                c_member(j, at_layer, step).wait_recv()
                if step + 1 < span - 1:
                    c_member(j, at_layer, step + 1).start()
        for bit in bits:
            c_aux(j, 0, bit).start()

    def finish_c(j):
        for k in sorted(range(1, aux), key=lambda k: -(k & -k)):
            c_aux(j, k ^ (k & -k), k & -k).wait_recv()
            for bit in lower(k):
                c_aux(j, k, bit).start()

    def transform(j, piece):
        @pl.when(piece == 0)
        def _():
            finish_c(j)
            h_acc[...] = jnp.zeros_like(h_acc)

        def block(i):
            h_acc[...] += jnp.dot(
                b[:, pl.ds(pl.multiple_of(i * n_rows, n_rows), n_rows)], c[j, i], preferred_element_type=jnp.float32)

        loop_from(lax.div(piece * rows_axis, pieces), lax.div((piece + 1) * rows_axis, pieces), block)

        @pl.when(piece == pieces - 1)
        def _():
            h[0, j, :, lanes(0)] = h_acc[...].astype(h.dtype)
            for bit in bits:
                h_aux(j, 0, bit).start()

            @pl.when(transit_far == 0)
            def _():
                loop(PARTS, lambda i: t_member(j, i).start())

            @pl.when(j > 0)
            def _():
                send_rest(j - 1)

            send_first(j)

            @pl.when(j + 2 < chunks)
            def _():
                spread_c(j + 2)

    def pass_member(j, i):
        @pl.when(jnp.logical_not(other_by_transit(i)))
        def _():
            h_member(j, i, 0).start()

    def pass_line(j, i, way):
        is_far = main_up if way else jnp.logical_not(main_up)

        @pl.when(jnp.logical_and(up if way else down, jnp.logical_not(jnp.logical_and(is_far, own_by_transit(i)))))
        def _():
            h_line(j, i, way).start()

    def send_h(j, k):
        @pl.when(owner)
        def _():
            def send(i):
                pass_line(j, i, 1)
                pass_line(j, i, 0)
                pass_member(j, i)

            loop_from(k * PARTS, (k + 1) * PARTS, send)

    def take_h(j, k):
        h_aux(j, k ^ (k & -k), k & -k).wait_recv()
        for bit in lower(k):
            h_aux(j, k, bit).start()
        send_h(j, k)

    def send_first(j):
        send_h(j, 0)
        for k in range(1, aux // 2):
            take_h(j, k)

    def send_rest(j):
        for k in range(aux // 2, aux):
            take_h(j, k)

    def relay_h(j, i):
        @pl.when(layer > p)
        def _():
            h_line(j, i, 1).wait_recv()
            pass_line(j, i, 1)
            pass_member(j, i)

        @pl.when(layer < p)
        def _():
            h_line(j, i, 0).wait_recv()
            pass_line(j, i, 0)
            pass_member(j, i)

    def relay_t(j, i):
        is_first = transit_far == 0
        is_other = i < PARTS

        @pl.when(jnp.logical_or(transit_far > 0, jnp.logical_and(is_first, is_other)))
        def _():
            t_line(t.at[j, i], j, i).wait_recv()

            @pl.when(transit_on)
            def _():
                t_line(t.at[j, i], j, i).start()

            @pl.when(is_other)
            def _():
                t_other(j, i).start()

            @pl.when(jnp.logical_not(is_other))
            def _():
                t_own(j, i).start()

        @pl.when(jnp.logical_and(jnp.logical_and(is_first, transit_on), jnp.logical_not(is_other)))
        def _():
            t_line(message(0, j, i), j, i).start()

    tile = min(TILE, n_rows)
    tiles = n_rows // tile
    all_tiles = span * tiles

    def take_members(j, first, last):
        for step in range(span - 1):
            def take(i):
                h_member(j, i, step).wait_recv()
                if step + 1 < span - 1:
                    h_member(j, i, step + 1).start()
            loop_from(first, last, take)

    def add_tile(j, n, first, last):
        line = lax.div(n, tiles)
        slot = jnp.where(line == member, own_slot, 1 + line)
        at = pl.ds(pl.multiple_of(lax.rem(n, tiles) * tile, tile), tile)
        some = pl.ds(first * width, (last - first) * width)
        k_acc[:, pl.ds(pl.multiple_of(n * tile, tile), tile)] += lax.dot_general(
            h[0, j, :, some], h[slot, j, at, some], (((1,), (1,)), ((), ())), preferred_element_type=jnp.float32)

    def update(j, piece, count):
        @pl.when(piece == 0)
        def _():
            take_members(j, 0, slots)

        loop_from(lax.div(piece * all_tiles, count), lax.div((piece + 1) * all_tiles, count),
                  lambda n: add_tile(j, n, 0, aux))

    def last_update(j):
        take_members(j, 0, slots - PARTS)
        loop(all_tiles, lambda n: add_tile(j, n, 0, aux - 1))
        take_members(j, slots - PARTS, slots)

        def finish(n):
            add_tile(j, n, aux - 1, aux)

        loop(all_tiles, finish)

    loop(chunks, start_c)

    def clear(n):
        columns = pl.ds(pl.multiple_of(n * tile, tile), tile)
        k_acc[:, columns] = jnp.zeros((n_rows, tile), jnp.float32)

    loop(span * tiles, clear)

    relay_c(0)
    relay_c(1)
    spread_c(0)
    relay_c(2)
    spread_c(1)
    loop(chunks - 3, lambda i: relay_c(i + 3))
    load_b.wait()
    loop(pieces, lambda piece: transform(0, piece))

    @pl.when(transit_far == 0)
    def _():
        loop(TRANSIT, lambda i: relay_t(0, i))

    quarter = slots // 4

    def main(j):
        def slot(i):
            relay_h(j, i)

            turn = j * slots + i + slots - pieces - TRANSIT * transit_far
            opening = i - jnp.minimum(TRANSIT * (transit_far - 1), slots - TRANSIT)
            is_opening = jnp.logical_and(
                jnp.logical_and(j == 0, transit_far > 0), jnp.logical_and(opening >= 0, opening < TRANSIT))
            t_chunk = jnp.where(is_opening, 0, lax.div(jnp.maximum(turn, 0), slots))
            t_message = jnp.where(is_opening, opening, lax.rem(jnp.maximum(turn, 0), slots))
            t_now = jnp.logical_or(is_opening, jnp.logical_and(
                jnp.logical_and(turn >= slots, t_chunk < chunks), t_message < TRANSIT))

            @pl.when(jnp.logical_and(t_now, transit_far >= 0))
            def _():
                relay_t(t_chunk, t_message)

            early = jnp.logical_and(j == 1, i < quarter)
            chunk = jnp.where(j == 0, jnp.where(i < pieces, 1, 2), jnp.where(early, 2, j + 2))
            piece = jnp.where(
                j == 0, jnp.where(i < pieces, i, i - 3 * quarter), jnp.where(early, i + quarter, i - quarter))
            now = jnp.logical_and(jnp.logical_and(piece >= 0, piece < pieces), chunk < chunks)

            @pl.when(now)
            def _():
                transform(chunk, piece)

            @pl.when(jnp.logical_and(j > 0, i >= 3 * quarter))
            def _():
                update(j - 1, i - 3 * quarter, quarter)

        loop(slots, slot)

        @pl.when(j == max(chunks - 2, 0))
        def _():
            send_rest(chunks - 1)

    loop(chunks, main)
    last_update(chunks - 1)

    def drain(j):
        for at_layer in range(aux):
            @pl.when(jnp.logical_and(up, at_layer <= layer))
            def _():
                c_line(j, at_layer, 1).wait_send()

            @pl.when(jnp.logical_and(down, at_layer >= layer))
            def _():
                c_line(j, at_layer, 0).wait_send()

            for step in range(span - 1):
                c_member(j, at_layer, step).wait_send()
        for k in range(1, aux):
            low = k & -k
            c_aux(j, k ^ low, low).wait_send()
            h_aux(j, k ^ low, low).wait_send()

        own_kept = slots - (last_transit - first_own)
        for way, has_next, sends in ((1, up, layer >= p), (0, down, layer <= p)):
            is_far = main_up if way else jnp.logical_not(main_up)

            @pl.when(jnp.logical_and(jnp.logical_and(has_next, sends), is_far))
            def _():
                h_line_sent(j, way, own_kept).wait_send()

            @pl.when(jnp.logical_and(jnp.logical_and(has_next, sends), jnp.logical_not(is_far)))
            def _():
                h_line_sent(j, way, slots).wait_send()

        @pl.when(main_far >= 0)
        def _():
            h_member_sent(j, 0, slots - PARTS).wait_send()

        @pl.when(main_far < 0)
        def _():
            h_member_sent(j, 0, slots).wait_send()

        for step in range(1, span - 1):
            h_member_sent(j, step, slots).wait_send()

        @pl.when(transit_far == 0)
        def _():
            t_sent(j, PARTS, ty_s, to_row(next_member)).wait_send()
            t_sent(j, PARTS, tx_s, to_aux(partner)).wait_send()

        @pl.when(transit_far > 0)
        def _():
            t_sent(j, TRANSIT, tx_s, to_aux(partner)).wait_send()

        @pl.when(transit_on)
        def _():
            t_sent(j, TRANSIT, tz_s, to_row(transit_row)).wait_send()

    loop(chunks, drain)


def body(aux, rows_axis, integrals, orbitals):
    _, n_rows, n = integrals.shape
    occ = orbitals.shape[1]
    span = rows_axis // aux
    width = CHUNK
    chunks = occ // width
    dma = pltpu.SemaphoreType.DMA
    tiles = span * (n_rows // min(TILE, n_rows))
    steps = max(span - 1, 1)
    return pl.pallas_call(
        functools.partial(kernel, aux, rows_axis),
        out_shape=pltpu.VMEM((n_rows, span * n_rows), jnp.float32),
        in_specs=[pl.BlockSpec(memory_space=pl.ANY)] * 2,
        out_specs=pl.BlockSpec(memory_space=pltpu.VMEM),
        scratch_shapes=[
            pltpu.VMEM((n_rows, n), integrals.dtype),
            pltpu.VMEM((chunks, rows_axis, n_rows, width), orbitals.dtype),
            pltpu.VMEM((1 + span, chunks, n_rows, aux * width), jnp.bfloat16),
            pltpu.VMEM((chunks, TRANSIT, n_rows // PARTS, width), jnp.bfloat16),
            pltpu.VMEM((n_rows, width), jnp.float32),
            dma, dma((chunks,)),
            dma((2, chunks, aux)), dma((chunks, aux)),
            dma((chunks, steps, aux)), dma((chunks, steps, aux)),
            dma((chunks, aux)), dma((chunks, aux)),
            dma((chunks, aux)), dma((chunks, aux)),
            dma((2, chunks)), dma((chunks, aux * PARTS)),
            dma((chunks, steps)), dma((chunks, steps, aux * PARTS)),
            dma((chunks,)), dma((chunks,)), dma((chunks,)), dma((chunks, TRANSIT)),
        ],
        compiler_params=pltpu.CompilerParams(
            collective_id=0, has_side_effects=True, vmem_limit_bytes=54 * 2**20),
    )(integrals.reshape(n_rows, n), orbitals)


def solution(mesh):
    aux, rows_axis = mesh.shape["aux"], mesh.shape["row"]
    return jax.shard_map(
        functools.partial(body, aux, rows_axis), mesh=mesh,
        in_specs=(P("aux", "row", None), P("row", None)), out_specs=P("row", "aux"), check_vma=False)
```

```python
import functools

import jax
import jax.numpy as jnp
from jax import lax
from jax.experimental import pallas as pl
from jax.experimental.pallas import tpu as pltpu
from jax.sharding import PartitionSpec as P

MESH = pl.DeviceIdType.MESH
CHUNK = 128
TILE = 256
PARTS = 4


def kernel(aux, rows_axis, b_hbm, c_hbm, k_acc, b, c, h, h_acc, *sems):
    (local_b, local_c, cz_s, cz_r, cy_s, cy_r, cx_s, cx_r,
     hx_s, hx_r, hz_s, hz_r, hy_s, hy_r) = sems
    span = rows_axis // aux
    chunks, _, _, n_rows, width = c.shape
    share = n_rows // aux
    p = lax.axis_index("aux")
    r = lax.axis_index("row")
    layer = lax.div(r, span)
    member = lax.rem(r, span)
    bits = []
    bit = aux // 2
    while bit:
        bits.append(bit)
        bit //= 2

    def row_of(at_layer, at_member):
        return at_layer * span + at_member

    next_member = row_of(layer, lax.rem(member + 1, span))
    last_member = row_of(layer, lax.rem(member + span - 1, span))
    owner = layer == p
    own_slot = jnp.where(owner, 0, 1 + member)

    def to_row(row):
        return {"device_id": {"row": row}, "device_id_type": MESH}

    def to_aux(index):
        return {"device_id": {"aux": index}, "device_id_type": MESH}

    def lower(k):
        low = k & -k if k else aux
        return [bit for bit in bits if bit < low]

    def quarter_of(index):
        return pl.ds(pl.multiple_of(index * share, share), share)

    def c_piece(j, at_layer, at_member):
        return c.at[j, at_layer, at_member, quarter_of(p)]

    def c_line(j, at_layer, way):
        piece = c_piece(j, at_layer, member)
        return pltpu.make_async_remote_copy(
            piece, piece, cz_s.at[way], cz_r.at[j, at_layer], **to_row(row_of(layer + 2 * way - 1, member)))

    def c_line_sent(way, count):
        some = c.at[:, 0, 0, pl.ds(0, count * share)]
        return pltpu.make_async_remote_copy(
            some, some, cz_s.at[way], cz_r.at[0, 0], **to_row(row_of(layer + 2 * way - 1, member)))

    def c_member(j, at_layer, step):
        piece = c_piece(j, at_layer, lax.rem(member + span - step, span))
        return pltpu.make_async_remote_copy(
            piece, piece, cy_s.at[step], cy_r.at[j, step], **to_row(next_member))

    def c_members(j, step):
        pieces = c.at[j, :, 0, quarter_of(p)]
        return pltpu.make_async_remote_copy(
            pieces, pieces, cy_s.at[step], cy_r.at[j, step], **to_row(next_member))

    def c_members_sent(step):
        some = c.at[:, 0, 0]
        return pltpu.make_async_remote_copy(some, some, cy_s.at[step], cy_r.at[0, step], **to_row(next_member))

    def c_aux_copy(piece, j, k, bit):
        return pltpu.make_async_remote_copy(
            piece, piece, cx_s, cx_r.at[j, k ^ bit], **to_aux(jnp.bitwise_xor(p, bit)))

    def c_aux_piece(j, at_layer, bit):
        return c_aux_copy(c_piece(j, at_layer, member), j, 0, bit)

    def c_aux_members(j, at_member, bit):
        return c_aux_copy(c.at[j, :, at_member, quarter_of(p)], j, 0, bit)

    def c_aux(j, k, bit):
        return c_aux_copy(c.at[j, :, :, quarter_of(jnp.bitwise_xor(p, k))], j, k, bit)

    def c_aux_sent():
        some = c.at[:, :, :, pl.ds(0, (aux - 1) * share)]
        return pltpu.make_async_remote_copy(some, some, cx_s, cx_r.at[0, 0], **to_aux(jnp.bitwise_xor(p, 1)))

    def lanes(k):
        return pl.ds(k * width, width)

    def h_aux(j, k, bit):
        return pltpu.make_async_remote_copy(
            h.at[0, j, :, lanes(k)], h.at[0, j, :, lanes(k ^ bit)], hx_s, hx_r.at[j, k ^ bit],
            **to_aux(jnp.bitwise_xor(p, bit)))

    def h_aux_sent():
        some = h.at[0, :, :, pl.ds(0, (aux - 1) * width)]
        return pltpu.make_async_remote_copy(some, some, hx_s, hx_r.at[0, 0], **to_aux(jnp.bitwise_xor(p, 1)))

    part = n_rows // PARTS
    slots = aux * PARTS
    pieces = slots // 2

    def message(slot, j, i):
        rows = pl.ds(pl.multiple_of(lax.rem(i, PARTS) * part, part), part)
        return h.at[slot, j, rows, pl.ds(pl.multiple_of(lax.div(i, PARTS) * width, width), width)]

    def h_line(j, i, way):
        return pltpu.make_async_remote_copy(
            message(own_slot, j, i), message(1 + member, j, i), hz_s.at[way], hz_r.at[j, i],
            **to_row(row_of(layer + 2 * way - 1, member)))

    def h_line_sent(way):
        return pltpu.make_async_remote_copy(
            h.at[0], h.at[0], hz_s.at[way], hz_r.at[0, 0], **to_row(row_of(layer + 2 * way - 1, member)))

    def h_member(j, i, step):
        line = lax.rem(member + span - step, span)
        slot = own_slot if step == 0 else 1 + line
        return pltpu.make_async_remote_copy(
            message(slot, j, i), message(1 + line, j, i), hy_s.at[step], hy_r.at[j, step, lax.div(i, pieces)],
            **to_row(next_member))

    def h_members(j, half, step):
        some = h.at[0, j, :, pl.ds(0, aux // 2 * width)]
        return pltpu.make_async_remote_copy(some, some, hy_s.at[step], hy_r.at[j, step, half], **to_row(next_member))

    def h_member_sent(step):
        return pltpu.make_async_remote_copy(
            h.at[0], h.at[0], hy_s.at[step], hy_r.at[0, step, 0], **to_row(next_member))

    up, down = layer + 1 < aux, layer > 0

    barrier = pltpu.get_barrier_semaphore()
    for bit in bits:
        pl.semaphore_signal(barrier, 1, **to_aux(jnp.bitwise_xor(p, bit)))
    pl.semaphore_signal(barrier, 1, **to_row(next_member))
    pl.semaphore_signal(barrier, 1, **to_row(last_member))

    @pl.when(up)
    def _():
        pl.semaphore_signal(barrier, 1, **to_row(row_of(layer + 1, member)))

    @pl.when(down)
    def _():
        pl.semaphore_signal(barrier, 1, **to_row(row_of(layer - 1, member)))

    def own_c(j):
        return pltpu.make_async_copy(
            c_hbm.at[pl.ds(pl.multiple_of(p * share, share), share), pl.ds(pl.multiple_of(j * width, width), width)],
            c_piece(j, layer, member), local_c.at[j])

    for j in range(chunks):
        own_c(j).start()
    load_b = pltpu.make_async_copy(b_hbm, b, local_b)
    load_b.start()
    pl.semaphore_wait(barrier, len(bits) + 2 + up.astype(jnp.int32) + down.astype(jnp.int32))

    def loop_from(first, last, body):
        def step(i, carry):
            body(i)
            return carry
        lax.fori_loop(first, last, step, 0)

    def loop(count, body):
        loop_from(0, count, body)

    def pass_c(j, at_layer, spread):
        c_member(j, at_layer, 0).start()
        if spread:
            for bit in bits:
                c_aux_piece(j, at_layer, bit).start()

    def start_c(j, spread=False):
        own_c(j).wait()

        @pl.when(up)
        def _():
            c_line(j, layer, 1).start()

        @pl.when(down)
        def _():
            c_line(j, layer, 0).start()

        pass_c(j, layer, spread)

    def relay_c(j, spread=False):
        for step in range(1, aux):
            @pl.when(layer - step >= 0)
            def _():
                c_line(j, layer - step, 1).wait_recv()

                @pl.when(up)
                def _():
                    c_line(j, layer - step, 1).start()

                pass_c(j, layer - step, spread)

            @pl.when(layer + step < aux)
            def _():
                c_line(j, layer + step, 0).wait_recv()

                @pl.when(down)
                def _():
                    c_line(j, layer + step, 0).start()

                pass_c(j, layer + step, spread)

    def spread_c(j, spread=False):
        if not spread:
            for bit in bits:
                c_aux_members(j, member, bit).start()
        for step in range(span - 1):
            c_members(j, step).wait_recv()
            if step + 1 < span - 1:
                for at_layer in range(aux):
                    c_member(j, at_layer, step + 1).start()
            for bit in bits:
                c_aux_members(j, lax.rem(member + span - 1 - step, span), bit).start()

    def finish_c(j):
        for k in sorted(range(1, aux), key=lambda k: -(k & -k)):
            c_aux(j, k ^ (k & -k), k & -k).wait_recv()
            for bit in lower(k):
                c_aux(j, k, bit).start()

    slots = aux * PARTS
    pieces = slots // 2

    def transform(j, piece):
        @pl.when(piece == 0)
        def _():
            finish_c(j)
            h_acc[...] = jnp.zeros_like(h_acc)

        def block(i):
            h_acc[...] += jnp.dot(
                b[:, pl.ds(pl.multiple_of(i * n_rows, n_rows), n_rows)], c[j, lax.div(i, span), lax.rem(i, span)],
                preferred_element_type=jnp.float32)

        loop_from(lax.div(piece * rows_axis, pieces), lax.div((piece + 1) * rows_axis, pieces), block)

        @pl.when(piece == pieces - 1)
        def _():
            h[0, j, :, lanes(0)] = h_acc[...].astype(h.dtype)
            for bit in bits:
                h_aux(j, 0, bit).start()

            @pl.when(j > 0)
            def _():
                send_rest(j - 1)

            send_first(j)

            @pl.when(j + 2 < chunks)
            def _():
                spread_c(j + 2)

    def send_h(j, k):
        @pl.when(owner)
        def _():
            def send(i):
                @pl.when(up)
                def _():
                    h_line(j, i, 1).start()

                @pl.when(down)
                def _():
                    h_line(j, i, 0).start()

                h_member(j, i, 0).start()

            loop_from(k * PARTS, (k + 1) * PARTS, send)

    def take_h(j, k):
        h_aux(j, k ^ (k & -k), k & -k).wait_recv()
        for bit in lower(k):
            h_aux(j, k, bit).start()
        send_h(j, k)

    def send_first(j):
        send_h(j, 0)
        for k in range(1, aux // 2):
            take_h(j, k)

    def send_rest(j):
        for k in range(aux // 2, aux):
            take_h(j, k)

    def relay_h(j, i):
        @pl.when(layer > p)
        def _():
            h_line(j, i, 1).wait_recv()

            @pl.when(up)
            def _():
                h_line(j, i, 1).start()

            h_member(j, i, 0).start()

        @pl.when(layer < p)
        def _():
            h_line(j, i, 0).wait_recv()

            @pl.when(down)
            def _():
                h_line(j, i, 0).start()

            h_member(j, i, 0).start()

    tile = min(TILE, n_rows)
    tiles = n_rows // tile
    all_tiles = span * tiles

    def take_members(j, half):
        for step in range(span - 1):
            h_members(j, half, step).wait_recv()
            if step + 1 < span - 1:
                loop_from(half * pieces, (half + 1) * pieces, lambda i: h_member(j, i, step + 1).start())

    def add_tile(j, n, first, last):
        line = lax.div(n, tiles)
        slot = jnp.where(line == member, own_slot, 1 + line)
        at = pl.ds(pl.multiple_of(lax.rem(n, tiles) * tile, tile), tile)
        some = pl.ds(first * width, (last - first) * width)
        k_acc[:, pl.ds(pl.multiple_of(n * tile, tile), tile)] += lax.dot_general(
            h[0, j, :, some], h[slot, j, at, some], (((1,), (1,)), ((), ())), preferred_element_type=jnp.float32)

    def update(j, piece, count, halves):
        @pl.when(piece == 0)
        def _():
            for half in halves:
                take_members(j, half)

        loop_from(lax.div(piece * all_tiles, count), lax.div((piece + 1) * all_tiles, count),
                  lambda n: add_tile(j, n, halves[0] * (aux // 2), (halves[-1] + 1) * (aux // 2)))

    def last_update(j):
        def own(n):
            add_tile(j, member * tiles + n, aux // 2, aux)

        def other(n):
            add_tile(j, lax.rem(member * tiles + n, all_tiles), aux // 2, aux)

        loop(tiles, own)
        take_members(j, 1)
        loop_from(tiles, all_tiles, other)

    start_c(0, True)
    start_c(1, True)

    def clear(n):
        columns = pl.ds(pl.multiple_of(n * tile, tile), tile)
        k_acc[:, columns] = jnp.zeros((n_rows, tile), jnp.float32)

    loop(span * tiles, clear)

    relay_c(0, True)
    start_c(2)
    relay_c(1, True)
    spread_c(0, True)
    start_c(3)
    relay_c(2)
    spread_c(1, True)
    loop_from(4, chunks, start_c)
    relay_c(3)
    load_b.wait()
    loop(pieces // 2, lambda piece: transform(0, piece))
    loop_from(4, chunks - 1, relay_c)
    loop_from(pieces // 2, pieces, lambda piece: transform(0, piece))
    loop_from(max(4, chunks - 1), chunks, relay_c)

    quarter = slots // 4

    def main(j):
        def slot(i):
            relay_h(j, i)
            early = jnp.logical_and(j == 1, i < quarter)
            chunk = jnp.where(j == 0, jnp.where(i < pieces, 1, 2), jnp.where(early, 2, j + 2))
            piece = jnp.where(
                j == 0, jnp.where(i < pieces, i, i - 3 * quarter), jnp.where(early, i + quarter, i - quarter))
            now = jnp.logical_and(jnp.logical_and(piece >= 0, piece < pieces), chunk < chunks)

            @pl.when(now)
            def _():
                transform(chunk, piece)

            @pl.when(jnp.logical_and(jnp.logical_and(j > 0, j < chunks - 2), i >= 3 * quarter))
            def _():
                update(j - 1, i - 3 * quarter, quarter, (0, 1))

            @pl.when(jnp.logical_and(j >= chunks - 2, jnp.logical_and(i >= quarter, i < 3 * quarter)))
            def _():
                update(j - 1, i - quarter, pieces, (0, 1))

            @pl.when(jnp.logical_and(j == chunks - 1, i >= 3 * quarter))
            def _():
                update(j, i - 3 * quarter, quarter, (0,))

        loop(slots, slot)

        @pl.when(j == max(chunks - 2, 0))
        def _():
            send_rest(chunks - 1)

    loop(chunks, main)
    last_update(chunks - 1)

    for at in range(aux):
        @pl.when(layer == at)
        def _():
            if at + 1 < aux:
                c_line_sent(1, at + 1).wait_send()
            if at > 0:
                c_line_sent(0, aux - at).wait_send()
    c_aux_sent().wait_send()
    h_aux_sent().wait_send()
    for step in range(span - 1):
        c_members_sent(step).wait_send()
        h_member_sent(step).wait_send()

    @pl.when(jnp.logical_and(up, layer >= p))
    def _():
        h_line_sent(1).wait_send()

    @pl.when(jnp.logical_and(down, layer <= p))
    def _():
        h_line_sent(0).wait_send()


def body(aux, rows_axis, integrals, orbitals):
    _, n_rows, n = integrals.shape
    occ = orbitals.shape[1]
    span = rows_axis // aux
    width = CHUNK
    chunks = occ // width
    dma = pltpu.SemaphoreType.DMA
    tiles = span * (n_rows // min(TILE, n_rows))
    steps = max(span - 1, 1)
    return pl.pallas_call(
        functools.partial(kernel, aux, rows_axis),
        out_shape=pltpu.VMEM((n_rows, span * n_rows), jnp.float32),
        in_specs=[pl.BlockSpec(memory_space=pl.ANY)] * 2,
        out_specs=pl.BlockSpec(memory_space=pltpu.VMEM),
        scratch_shapes=[
            pltpu.VMEM((n_rows, n), integrals.dtype),
            pltpu.VMEM((chunks, aux, span, n_rows, width), orbitals.dtype),
            pltpu.VMEM((1 + span, chunks, n_rows, aux * width), jnp.bfloat16),
            pltpu.VMEM((n_rows, width), jnp.float32),
            dma, dma((chunks,)),
            dma((2,)), dma((chunks, aux)),
            dma((steps,)), dma((chunks, steps)),
            dma, dma((chunks, aux)),
            dma, dma((chunks, aux)),
            dma((2,)), dma((chunks, aux * PARTS)),
            dma((steps,)), dma((chunks, steps, 2)),
        ],
        compiler_params=pltpu.CompilerParams(
            collective_id=0, has_side_effects=True, vmem_limit_bytes=54 * 2**20),
    )(integrals.reshape(n_rows, n), orbitals)


def solution(mesh):
    aux, rows_axis = mesh.shape["aux"], mesh.shape["row"]
    return jax.shard_map(
        functools.partial(body, aux, rows_axis), mesh=mesh,
        in_specs=(P("aux", "row", None), P("row", None)), out_specs=P("row", "aux"), check_vma=False)
```

```python
import functools

import jax
import jax.numpy as jnp
from jax import lax
from jax.experimental import pallas as pl
from jax.experimental.pallas import tpu as pltpu
from jax.sharding import PartitionSpec as P

MESH = pl.DeviceIdType.MESH
CHUNK = 128
TILE = 256
PARTS = 4
REST = 5
TRANSIT_FROM = 3


def kernel(aux, rows_axis, b_hbm, c_hbm, k_acc, b, c, h, t, h_acc, *sems):
    (local_b, local_c, cz_s, cz_r, cy_s, cy_r, cx_s, cx_r,
     hx_s, hx_r, hz_s, hz_r, hy_s, hy_r, td_s, ty_s, t_r) = sems
    span = rows_axis // aux
    chunks, _, _, n_rows, width = c.shape
    share = n_rows // aux
    p = lax.axis_index("aux")
    r = lax.axis_index("row")
    layer = lax.div(r, span)
    member = lax.rem(r, span)
    bits = []
    bit = aux // 2
    while bit:
        bits.append(bit)
        bit //= 2

    def row_of(at_layer, at_member):
        return at_layer * span + at_member

    next_member = row_of(layer, lax.rem(member + 1, span))
    last_member = row_of(layer, lax.rem(member + span - 1, span))
    owner = layer == p
    own_slot = jnp.where(owner, 0, 1 + member)

    half = aux // 2
    partner = jnp.bitwise_xor(p, half)
    t_from = TRANSIT_FROM

    def ahead(index):
        return jnp.where(index < half, layer - index, index - layer)

    main_far, transit_far = ahead(p), ahead(partner)
    main_up = p < half

    def is_far_way(way):
        return main_up if way else jnp.logical_not(main_up)

    def to_row(row):
        return {"device_id": {"row": row}, "device_id_type": MESH}

    def to_aux(index):
        return {"device_id": {"aux": index}, "device_id_type": MESH}

    def lower(k):
        low = k & -k if k else aux
        return [bit for bit in bits if bit < low]

    def quarter_of(index):
        return pl.ds(pl.multiple_of(index * share, share), share)

    def c_piece(j, at_layer, at_member):
        return c.at[j, at_layer, at_member, quarter_of(p)]

    def c_line(j, at_layer, way):
        piece = c_piece(j, at_layer, member)
        return pltpu.make_async_remote_copy(
            piece, piece, cz_s.at[way], cz_r.at[j, at_layer], **to_row(row_of(layer + 2 * way - 1, member)))

    def c_direct(at_layer):
        piece = c_piece(0, layer, member)
        return pltpu.make_async_remote_copy(
            piece, piece, cz_s.at[2], cz_r.at[0, layer], **to_row(row_of(at_layer, member)))

    def c_direct_sent():
        some = c.at[0, 0, 0, pl.ds(0, (aux - 1) * share)]
        return pltpu.make_async_remote_copy(some, some, cz_s.at[2], cz_r.at[0, 0], **to_row(next_member))

    def c_line_sent(way, count):
        some = c.at[pl.ds(1, chunks - 1), 0, 0, pl.ds(0, count * share)]
        return pltpu.make_async_remote_copy(
            some, some, cz_s.at[way], cz_r.at[0, 0], **to_row(row_of(layer + 2 * way - 1, member)))

    def c_member(j, at_layer, step):
        piece = c_piece(j, at_layer, lax.rem(member + span - step, span))
        return pltpu.make_async_remote_copy(
            piece, piece, cy_s.at[step], cy_r.at[j, step], **to_row(next_member))

    def c_members(j, step):
        pieces = c.at[j, :, 0, quarter_of(p)]
        return pltpu.make_async_remote_copy(
            pieces, pieces, cy_s.at[step], cy_r.at[j, step], **to_row(next_member))

    def c_members_sent(step):
        some = c.at[:, 0, 0]
        return pltpu.make_async_remote_copy(some, some, cy_s.at[step], cy_r.at[0, step], **to_row(next_member))

    def c_aux_copy(piece, j, others, k, bit):
        return pltpu.make_async_remote_copy(
            piece, piece, cx_s, cx_r.at[j, others, k ^ bit], **to_aux(jnp.bitwise_xor(p, bit)))

    def c_aux_piece(j, at_layer, bit):
        return c_aux_copy(c_piece(j, at_layer, member), j, 0, 0, bit)

    def c_aux_members(j, step, k, bit):
        at_member = lax.rem(member + span - step, span)
        return c_aux_copy(c.at[j, :, at_member, quarter_of(jnp.bitwise_xor(p, k))], j, int(step > 0), k, bit)

    def c_aux_all(j, others, k, bit):
        some = c.at[j, :, pl.ds(0, span - 1 if others else 1), quarter_of(p)]
        return c_aux_copy(some, j, others, k, bit)

    def c_aux_sent():
        some = c.at[:, :, :, pl.ds(0, (aux - 1) * share)]
        return pltpu.make_async_remote_copy(some, some, cx_s, cx_r.at[0, 0, 0], **to_aux(jnp.bitwise_xor(p, 1)))

    def lanes(k):
        return pl.ds(k * width, width)

    def h_aux(j, k, bit):
        return pltpu.make_async_remote_copy(
            h.at[0, j, :, lanes(k)], h.at[0, j, :, lanes(k ^ bit)], hx_s, hx_r.at[j, k ^ bit],
            **to_aux(jnp.bitwise_xor(p, bit)))

    def h_aux_sent():
        some = h.at[0, :, :, pl.ds(0, (aux - 1) * width)]
        return pltpu.make_async_remote_copy(some, some, hx_s, hx_r.at[0, 0], **to_aux(jnp.bitwise_xor(p, 1)))

    part = n_rows // PARTS
    slots = aux * PARTS
    pieces = slots // 2

    def message(slot, j, i):
        rows = pl.ds(pl.multiple_of(lax.rem(i, PARTS) * part, part), part)
        return h.at[slot, j, rows, pl.ds(pl.multiple_of(lax.div(i, PARTS) * width, width), width)]

    def late(j):
        return int(j >= t_from) if isinstance(j, int) else (j >= t_from).astype(jnp.int32)

    def by_transit(j, i):
        return jnp.logical_and(j >= t_from, jnp.logical_and(i >= half * PARTS, i < (half + 1) * PARTS))

    def h_line(j, i, way):
        return pltpu.make_async_remote_copy(
            message(own_slot, j, i), message(1 + member, j, i), hz_s.at[way, late(j)], hz_r.at[j, i],
            **to_row(row_of(layer + 2 * way - 1, member)))

    def h_line_sent(way, is_late, count):
        some = h.at[0, pl.ds(t_from, chunks - t_from) if is_late else pl.ds(0, t_from), :, pl.ds(0, count * width)]
        return pltpu.make_async_remote_copy(
            some, some, hz_s.at[way, is_late], hz_r.at[0, 0], **to_row(row_of(layer + 2 * way - 1, member)))

    def h_member(j, i, step):
        line = lax.rem(member + span - step, span)
        slot = own_slot if step == 0 else 1 + line
        return pltpu.make_async_remote_copy(
            message(slot, j, i), message(1 + line, j, i), hy_s.at[step, late(j)], hy_r.at[j, step, lax.div(i, pieces)],
            **to_row(next_member))

    def h_members(j, half, step):
        some = h.at[0, j, :, pl.ds(0, aux // 2 * width)]
        return pltpu.make_async_remote_copy(some, some, hy_s.at[step, 0], hy_r.at[j, step, half], **to_row(next_member))

    def h_member_sent(step, is_late, count):
        some = h.at[0, pl.ds(t_from, chunks - t_from) if is_late else pl.ds(0, t_from), :, pl.ds(0, count * width)]
        return pltpu.make_async_remote_copy(
            some, some, hy_s.at[step, is_late], hy_r.at[0, step, 0], **to_row(next_member))

    def t_member(j):
        return pltpu.make_async_remote_copy(
            h.at[0, j, :, lanes(0)], t.at[j - t_from], ty_s, t_r.at[j - t_from], **to_row(next_member))

    def t_member_sent():
        return pltpu.make_async_remote_copy(t, t, ty_s, t_r.at[0], **to_row(next_member))

    def far_layer(distance):
        return jnp.where(partner < half, partner + distance, partner - distance)

    def to_far(distance):
        return {"device_id": {"aux": partner, "row": row_of(far_layer(distance), member)}, "device_id_type": MESH}

    def t_own(j, distance):
        return pltpu.make_async_remote_copy(
            h.at[0, j, :, lanes(0)], h.at[1 + member, j, :, lanes(half)], td_s.at[j - t_from],
            hz_r.at[j, half * PARTS], **to_far(distance))

    def t_other(j, distance):
        return pltpu.make_async_remote_copy(
            t.at[j - t_from], h.at[1 + lax.rem(member + span - 1, span), j, :, lanes(half)], td_s.at[j - t_from],
            hy_r.at[j, 0, 1], **to_far(distance))

    def t_sent(j, count):
        some = h.at[pl.ds(0, 2), 0, :, pl.ds(0, count * width)]
        return pltpu.make_async_remote_copy(some, some, td_s.at[j - t_from], t_r.at[0], **to_far(0))

    def each_far(body):
        for distance in range(aux - 1, 0, -1):
            at = far_layer(distance)

            @pl.when(jnp.logical_and(transit_far == 0, jnp.logical_and(at >= 0, at < aux)))
            def _():
                body(distance)

    up, down = layer + 1 < aux, layer > 0

    barrier = pltpu.get_barrier_semaphore()
    for bit in bits:
        pl.semaphore_signal(barrier, 1, **to_aux(jnp.bitwise_xor(p, bit)))
    pl.semaphore_signal(barrier, 1, **to_row(last_member))
    for step in range(1, aux):
        pl.semaphore_signal(barrier, 1, **to_row(row_of(lax.rem(layer + step, aux), member)))

    @pl.when(main_far > 0)
    def _():
        pl.semaphore_signal(
            barrier, 1, device_id={"aux": partner, "row": row_of(p, member)}, device_id_type=MESH)

    n_far = jnp.where(transit_far == 0, jnp.where(partner < half, aux - 1 - partner, partner), 0)

    def own_c(j):
        return pltpu.make_async_copy(
            c_hbm.at[pl.ds(pl.multiple_of(p * share, share), share), pl.ds(pl.multiple_of(j * width, width), width)],
            c_piece(j, layer, member), local_c.at[j])

    for j in range(chunks):
        own_c(j).start()
    load_b = pltpu.make_async_copy(b_hbm, b, local_b)
    load_b.start()
    pl.semaphore_wait(barrier, len(bits) + aux + n_far)

    def loop_from(first, last, body):
        def step(i, carry):
            body(i)
            return carry
        lax.fori_loop(first, last, step, 0)

    def loop(count, body):
        loop_from(0, count, body)

    def pass_c(j, at_layer, spread):
        c_member(j, at_layer, 0).start()
        if spread:
            for bit in bits:
                c_aux_piece(j, at_layer, bit).start()

    def first_c():
        own_c(0).wait()
        for step in range(1, aux):
            @pl.when(layer + step < aux)
            def _():
                c_direct(layer + step).start()

            @pl.when(layer - step >= 0)
            def _():
                c_direct(layer - step).start()

        pass_c(0, layer, True)

    def start_c(j, spread=False):
        own_c(j).wait()

        @pl.when(up)
        def _():
            c_line(j, layer, 1).start()

        @pl.when(down)
        def _():
            c_line(j, layer, 0).start()

        pass_c(j, layer, spread)

    def take_first_c():
        for step in range(1, aux):
            for at_layer in (layer - step, layer + step):
                @pl.when(jnp.logical_and(at_layer >= 0, at_layer < aux))
                def _():
                    c_line(0, at_layer, 0).wait_recv()
                    pass_c(0, at_layer, True)

    def relay_c(j, spread=False):
        for step in range(1, aux):

            @pl.when(layer - step >= 0)
            def _():
                c_line(j, layer - step, 1).wait_recv()

                @pl.when(up)
                def _():
                    c_line(j, layer - step, 1).start()

                pass_c(j, layer - step, spread)

            @pl.when(layer + step < aux)
            def _():
                c_line(j, layer + step, 0).wait_recv()

                @pl.when(down)
                def _():
                    c_line(j, layer + step, 0).start()

                pass_c(j, layer + step, spread)

    def spread_c(j, spread=False):
        if not spread:
            for bit in bits:
                c_aux_members(j, 0, 0, bit).start()
        for step in range(span - 1):
            c_members(j, step).wait_recv()
            if step + 1 < span - 1:
                for at_layer in range(aux):
                    c_member(j, at_layer, step + 1).start()
            for bit in bits:
                c_aux_members(j, step + 1, 0, bit).start()

    def finish_c(j, others):
        for k in sorted(range(1, aux), key=lambda k: -(k & -k)):
            c_aux_all(j, others, k ^ (k & -k), k & -k).wait_recv()
            for bit in lower(k):
                for step in range(1, span) if others else (0,):
                    c_aux_members(j, step, k, bit).start()

    def transform(j, piece):
        def block(at_layer, at_member):
            columns = pl.ds(pl.multiple_of(row_of(at_layer, at_member) * n_rows, n_rows), n_rows)
            h_acc[...] += jnp.dot(b[:, columns], c[j, at_layer, at_member], preferred_element_type=jnp.float32)

        middle = pieces // 2

        @pl.when(piece == 0)
        def _():
            finish_c(j, 0)
            h_acc[...] = jnp.zeros_like(h_acc)

        @pl.when(piece < middle)
        def _():
            loop_from(lax.div(piece * aux, middle), lax.div((piece + 1) * aux, middle), lambda i: block(i, member))

        @pl.when(piece == middle)
        def _():
            finish_c(j, 1)

        @pl.when(piece >= middle)
        def _():
            count = aux * (span - 1)
            loop_from(
                lax.div((piece - middle) * count, middle), lax.div((piece - middle + 1) * count, middle),
                lambda i: block(lax.rem(i, aux), lax.rem(member + 1 + lax.div(i, aux), span)))

        @pl.when(piece == pieces - 1)
        def _():
            h[0, j, :, lanes(0)] = h_acc[...].astype(h.dtype)
            for bit in bits:
                h_aux(j, 0, bit).start()

            if not isinstance(j, int) or j >= t_from:
                @pl.when(jnp.logical_and(j >= t_from, transit_far == 0))
                def _():
                    t_member(j).start()
                    each_far(lambda distance: t_own(j, distance).start())

            @pl.when(j > 1)
            def _():
                send_rest(j - 1)

            send_first(j)

            @pl.when(j + 2 < chunks)
            def _():
                spread_c(j + 2)

    def pass_member(j, i):
        @pl.when(jnp.logical_not(jnp.logical_and(main_far > 0, by_transit(j, i))))
        def _():
            h_member(j, i, 0).start()

    def pass_line(j, i, way):
        @pl.when(jnp.logical_and(up if way else down, jnp.logical_not(jnp.logical_and(is_far_way(way), by_transit(j, i)))))
        def _():
            h_line(j, i, way).start()

    def send_h(j, k):
        @pl.when(owner)
        def _():
            def send(i):
                pass_line(j, i, 1)
                pass_line(j, i, 0)
                pass_member(j, i)

            loop_from(k * PARTS, (k + 1) * PARTS, send)

    def take_h(j, k):
        h_aux(j, k ^ (k & -k), k & -k).wait_recv()
        for bit in lower(k):
            h_aux(j, k, bit).start()
        send_h(j, k)

    def send_first(j):
        send_h(j, 0)
        for k in range(1, aux // 2):
            take_h(j, k)

    def send_rest(j):
        for k in range(aux // 2, aux):
            take_h(j, k)

    def relay_h(j, i):
        for way in (1, 0):
            beyond = layer > p if way else layer < p

            @pl.when(jnp.logical_and(beyond, jnp.logical_not(jnp.logical_and(is_far_way(way), by_transit(j, i)))))
            def _():
                h_line(j, i, way).wait_recv()
                pass_line(j, i, way)
                pass_member(j, i)

    def relay_t(j):
        @pl.when(transit_far == 0)
        def _():
            t_member(j).wait_recv()
            each_far(lambda distance: t_other(j, distance).start())

    def take_own(j):
        @pl.when(jnp.logical_and(main_far > 0, j >= t_from))
        def _():
            t_own(jnp.maximum(j, t_from), 0).wait_recv()

    tile = min(TILE, n_rows)
    tiles = n_rows // tile
    all_tiles = span * tiles

    def take_members(j, half):
        for step in range(span - 1):
            h_members(j, half, step).wait_recv()
            if step + 1 < span - 1:
                loop_from(half * pieces, (half + 1) * pieces, lambda i: h_member(j, i, step + 1).start())

    def add_tile(j, n, first, last):
        line = lax.div(n, tiles)
        slot = jnp.where(line == member, own_slot, 1 + line)
        at = pl.ds(pl.multiple_of(lax.rem(n, tiles) * tile, tile), tile)
        some = pl.ds(first * width, (last - first) * width)
        k_acc[:, pl.ds(pl.multiple_of(n * tile, tile), tile)] += lax.dot_general(
            h[0, j, :, some], h[slot, j, at, some], (((1,), (1,)), ((), ())), preferred_element_type=jnp.float32)

    def update(j, piece, count, halves):
        @pl.when(piece == 0)
        def _():
            for half in halves:
                take_members(j, half)
            if 1 in halves:
                take_own(j)

        loop_from(lax.div(piece * all_tiles, count), lax.div((piece + 1) * all_tiles, count),
                  lambda n: add_tile(j, n, halves[0] * (aux // 2), (halves[-1] + 1) * (aux // 2)))

    def last_update(j):
        def own(n):
            add_tile(j, member * tiles + n, aux // 2, aux)

        def other(n):
            add_tile(j, lax.rem(member * tiles + n, all_tiles), aux // 2, aux)

        take_own(j)
        loop(tiles, own)
        take_members(j, 1)
        loop_from(tiles, all_tiles, other)

    first_c()

    def clear(n):
        columns = pl.ds(pl.multiple_of(n * tile, tile), tile)
        k_acc[:, columns] = jnp.zeros((n_rows, tile), jnp.float32)

    loop(span * tiles, clear)

    start_c(1)
    take_first_c()
    start_c(2)
    relay_c(1)
    spread_c(0, True)
    start_c(3)
    relay_c(2)
    loop_from(4, chunks, start_c)
    spread_c(1)
    load_b.wait()
    loop(pieces // 2, lambda piece: transform(0, piece))
    relay_c(3)
    loop_from(pieces // 2, pieces, lambda piece: transform(0, piece))
    loop_from(4, chunks, relay_c)

    quarter = slots // 4

    def main(j):
        def slot(i):
            relay_h(j, i)
            early = jnp.logical_and(j == 1, i < quarter)
            chunk = jnp.where(j == 0, jnp.where(i < pieces, 1, 2), jnp.where(early, 2, j + 2))
            piece = jnp.where(
                j == 0, jnp.where(i < pieces, i, i - 3 * quarter), jnp.where(early, i + quarter, i - quarter))

            @pl.when(jnp.logical_and(j + 1 >= t_from, jnp.logical_and(i == pieces, j + 1 < chunks)))
            def _():
                relay_t(j + 1)

            @pl.when(jnp.logical_and(j == 0, i == REST))
            def _():
                send_rest(0)

            now = jnp.logical_and(jnp.logical_and(piece >= 0, piece < pieces), chunk < chunks)

            @pl.when(now)
            def _():
                transform(chunk, piece)

            @pl.when(jnp.logical_and(jnp.logical_and(j > 0, j < chunks - 2), i >= 3 * quarter))
            def _():
                update(j - 1, i - 3 * quarter, quarter, (0, 1))

            @pl.when(jnp.logical_and(j >= chunks - 2, jnp.logical_and(i >= quarter, i < 3 * quarter)))
            def _():
                update(j - 1, i - quarter, pieces, (0, 1))

        loop(slots, slot)

        @pl.when(j == max(chunks - 2, 0))
        def _():
            send_rest(chunks - 1)

    loop(chunks, main)
    update(chunks - 1, 0, 1, (0,))
    last_update(chunks - 1)

    for at in range(aux):
        @pl.when(layer == at)
        def _():
            if at + 1 < aux:
                c_line_sent(1, at + 1).wait_send()
            if at > 0:
                c_line_sent(0, aux - at).wait_send()
    c_direct_sent().wait_send()
    c_aux_sent().wait_send()
    h_aux_sent().wait_send()
    for step in range(span - 1):
        c_members_sent(step).wait_send()
        h_member_sent(step, 0, aux).wait_send()
        fewer = jnp.logical_and(main_far > 0, step == 0)

        @pl.when(fewer)
        def _():
            h_member_sent(step, 1, aux - 1).wait_send()

        @pl.when(jnp.logical_not(fewer))
        def _():
            h_member_sent(step, 1, aux).wait_send()

    for way, has_next, sends in ((1, up, layer >= p), (0, down, layer <= p)):
        @pl.when(jnp.logical_and(has_next, sends))
        def _():
            h_line_sent(way, 0, aux).wait_send()

            @pl.when(is_far_way(way))
            def _():
                h_line_sent(way, 1, aux - 1).wait_send()

            @pl.when(jnp.logical_not(is_far_way(way)))
            def _():
                h_line_sent(way, 1, aux).wait_send()

    @pl.when(transit_far == 0)
    def _():
        t_member_sent().wait_send()

    for index in range(aux):
        @pl.when(jnp.logical_and(transit_far == 0, partner == index))
        def _():
            count = aux - 1 - index if index < half else index
            loop_from(t_from, chunks, lambda j: t_sent(j, count).wait_send())


def body(aux, rows_axis, integrals, orbitals):
    _, n_rows, n = integrals.shape
    occ = orbitals.shape[1]
    span = rows_axis // aux
    width = CHUNK
    chunks = occ // width
    dma = pltpu.SemaphoreType.DMA
    tiles = span * (n_rows // min(TILE, n_rows))
    steps = max(span - 1, 1)
    return pl.pallas_call(
        functools.partial(kernel, aux, rows_axis),
        out_shape=pltpu.VMEM((n_rows, span * n_rows), jnp.float32),
        in_specs=[pl.BlockSpec(memory_space=pl.ANY)] * 2,
        out_specs=pl.BlockSpec(memory_space=pltpu.VMEM),
        scratch_shapes=[
            pltpu.VMEM((n_rows, n), integrals.dtype),
            pltpu.VMEM((chunks, aux, span, n_rows, width), orbitals.dtype),
            pltpu.VMEM((1 + span, chunks, n_rows, aux * width), jnp.bfloat16),
            pltpu.VMEM((chunks - TRANSIT_FROM, n_rows, width), jnp.bfloat16),
            pltpu.VMEM((n_rows, width), jnp.float32),
            dma, dma((chunks,)),
            dma((3,)), dma((chunks, aux)),
            dma((steps,)), dma((chunks, steps)),
            dma, dma((chunks, 2, aux)),
            dma, dma((chunks, aux)),
            dma((2, 2)), dma((chunks, aux * PARTS)),
            dma((steps, 2)), dma((chunks, steps, 2)),
            dma((chunks - TRANSIT_FROM,)), dma, dma((chunks - TRANSIT_FROM,)),
        ],
        compiler_params=pltpu.CompilerParams(
            collective_id=0, has_side_effects=True, vmem_limit_bytes=54 * 2**20),
    )(integrals.reshape(n_rows, n), orbitals)


def solution(mesh):
    aux, rows_axis = mesh.shape["aux"], mesh.shape["row"]
    return jax.shard_map(
        functools.partial(body, aux, rows_axis), mesh=mesh,
        in_specs=(P("aux", "row", None), P("row", None)), out_specs=P("row", "aux"), check_vma=False)
```

```python
import functools

import jax
import jax.numpy as jnp
from jax import lax
from jax.experimental import pallas as pl
from jax.experimental.pallas import tpu as pltpu
from jax.sharding import PartitionSpec as P

MESH = pl.DeviceIdType.MESH
CHUNK = 128
TILE = 256
PARTS = 4
REST = 3
START = 6
LATER = 8
TRANSIT_FROM = 3


def kernel(aux, rows_axis, b_hbm, c_hbm, k_acc, b, c, h, t, h_acc, *sems):
    (local_b, local_c, cz_s, cz_r, cy_s, cy_r, cx_s, cx_r,
     hx_s, hx_r, hz_s, hz_r, hy_s, hy_r, td_s, ty_s, t_r) = sems
    span = rows_axis // aux
    chunks, _, _, n_rows, width = c.shape
    share = n_rows // aux
    p = lax.axis_index("aux")
    r = lax.axis_index("row")
    layer = lax.div(r, span)
    member = lax.rem(r, span)
    bits = []
    bit = aux // 2
    while bit:
        bits.append(bit)
        bit //= 2

    def row_of(at_layer, at_member):
        return at_layer * span + at_member

    next_member = row_of(layer, lax.rem(member + 1, span))
    last_member = row_of(layer, lax.rem(member + span - 1, span))
    owner = layer == p
    own_slot = jnp.where(owner, 0, 1 + member)

    half = aux // 2
    partner = jnp.bitwise_xor(p, half)
    t_from = TRANSIT_FROM

    def ahead(index):
        return jnp.where(index < half, layer - index, index - layer)

    main_far, transit_far = ahead(p), ahead(partner)
    main_up = p < half

    def is_far_way(way):
        return main_up if way else jnp.logical_not(main_up)

    def to_row(row):
        return {"device_id": {"row": row}, "device_id_type": MESH}

    def to_aux(index):
        return {"device_id": {"aux": index}, "device_id_type": MESH}

    def lower(k):
        low = k & -k if k else aux
        return [bit for bit in bits if bit < low]

    def quarter_of(index):
        return pl.ds(pl.multiple_of(index * share, share), share)

    def c_piece(j, at_layer, at_member):
        return c.at[j, at_layer, at_member, quarter_of(p)]

    def c_line(j, at_layer, way):
        piece = c_piece(j, at_layer, member)
        return pltpu.make_async_remote_copy(
            piece, piece, cz_s.at[way], cz_r.at[j, at_layer], **to_row(row_of(layer + 2 * way - 1, member)))

    def c_direct(at_layer):
        piece = c_piece(0, layer, member)
        return pltpu.make_async_remote_copy(
            piece, piece, cz_s.at[2], cz_r.at[0, layer], **to_row(row_of(at_layer, member)))

    def c_direct_sent():
        some = c.at[0, 0, 0, pl.ds(0, (aux - 1) * share)]
        return pltpu.make_async_remote_copy(some, some, cz_s.at[2], cz_r.at[0, 0], **to_row(next_member))

    def c_line_sent(way, count):
        some = c.at[pl.ds(1, chunks - 1), 0, 0, pl.ds(0, count * share)]
        return pltpu.make_async_remote_copy(
            some, some, cz_s.at[way], cz_r.at[0, 0], **to_row(row_of(layer + 2 * way - 1, member)))

    def c_member(j, at_layer, step):
        piece = c_piece(j, at_layer, lax.rem(member + span - step, span))
        return pltpu.make_async_remote_copy(
            piece, piece, cy_s.at[step], cy_r.at[j, step], **to_row(next_member))

    def c_members(j, step):
        pieces = c.at[j, :, 0, quarter_of(p)]
        return pltpu.make_async_remote_copy(
            pieces, pieces, cy_s.at[step], cy_r.at[j, step], **to_row(next_member))

    def c_members_sent(step):
        some = c.at[:, 0, 0]
        return pltpu.make_async_remote_copy(some, some, cy_s.at[step], cy_r.at[0, step], **to_row(next_member))

    def c_aux_copy(piece, j, others, k, bit):
        return pltpu.make_async_remote_copy(
            piece, piece, cx_s, cx_r.at[j, others, k ^ bit], **to_aux(jnp.bitwise_xor(p, bit)))

    def c_aux_piece(j, at_layer, bit):
        return c_aux_copy(c_piece(j, at_layer, member), j, 0, 0, bit)

    def c_aux_members(j, step, k, bit):
        at_member = lax.rem(member + span - step, span)
        return c_aux_copy(c.at[j, :, at_member, quarter_of(jnp.bitwise_xor(p, k))], j, int(step > 0), k, bit)

    def c_aux_all(j, others, k, bit):
        some = c.at[j, :, pl.ds(0, span - 1 if others else 1), quarter_of(p)]
        return c_aux_copy(some, j, others, k, bit)

    def c_aux_sent():
        some = c.at[:, :, :, pl.ds(0, (aux - 1) * share)]
        return pltpu.make_async_remote_copy(some, some, cx_s, cx_r.at[0, 0, 0], **to_aux(jnp.bitwise_xor(p, 1)))

    def lanes(k):
        return pl.ds(k * width, width)

    def h_aux(j, k, bit):
        return pltpu.make_async_remote_copy(
            h.at[0, j, :, lanes(k)], h.at[0, j, :, lanes(k ^ bit)], hx_s, hx_r.at[j, k ^ bit],
            **to_aux(jnp.bitwise_xor(p, bit)))

    def h_aux_sent():
        some = h.at[0, :, :, pl.ds(0, (aux - 1) * width)]
        return pltpu.make_async_remote_copy(some, some, hx_s, hx_r.at[0, 0], **to_aux(jnp.bitwise_xor(p, 1)))

    part = n_rows // PARTS
    slots = aux * PARTS
    pieces = slots // 2

    def message(slot, j, i):
        rows = pl.ds(pl.multiple_of(lax.rem(i, PARTS) * part, part), part)
        return h.at[slot, j, rows, pl.ds(pl.multiple_of(lax.div(i, PARTS) * width, width), width)]

    def late(j):
        return int(j >= t_from) if isinstance(j, int) else (j >= t_from).astype(jnp.int32)

    def by_transit(j, i):
        return jnp.logical_and(j >= t_from, jnp.logical_and(i >= half * PARTS, i < (half + 1) * PARTS))

    def h_line(j, i, way):
        return pltpu.make_async_remote_copy(
            message(own_slot, j, i), message(1 + member, j, i), hz_s.at[way, late(j)], hz_r.at[j, i],
            **to_row(row_of(layer + 2 * way - 1, member)))

    def h_line_sent(way, is_late, count):
        some = h.at[0, pl.ds(t_from, chunks - t_from) if is_late else pl.ds(0, t_from), :, pl.ds(0, count * width)]
        return pltpu.make_async_remote_copy(
            some, some, hz_s.at[way, is_late], hz_r.at[0, 0], **to_row(row_of(layer + 2 * way - 1, member)))

    def h_member(j, i, step):
        line = lax.rem(member + span - step, span)
        slot = own_slot if step == 0 else 1 + line
        return pltpu.make_async_remote_copy(
            message(slot, j, i), message(1 + line, j, i), hy_s.at[step, late(j)], hy_r.at[j, step, lax.div(i, pieces)],
            **to_row(next_member))

    def h_members(j, half, step):
        some = h.at[0, j, :, pl.ds(0, aux // 2 * width)]
        return pltpu.make_async_remote_copy(some, some, hy_s.at[step, 0], hy_r.at[j, step, half], **to_row(next_member))

    def h_member_sent(step, is_late, count):
        some = h.at[0, pl.ds(t_from, chunks - t_from) if is_late else pl.ds(0, t_from), :, pl.ds(0, count * width)]
        return pltpu.make_async_remote_copy(
            some, some, hy_s.at[step, is_late], hy_r.at[0, step, 0], **to_row(next_member))

    def t_member(j):
        return pltpu.make_async_remote_copy(
            h.at[0, j, :, lanes(0)], t.at[j - t_from], ty_s, t_r.at[j - t_from], **to_row(next_member))

    def t_member_sent():
        return pltpu.make_async_remote_copy(t, t, ty_s, t_r.at[0], **to_row(next_member))

    def far_layer(distance):
        return jnp.where(partner < half, partner + distance, partner - distance)

    def to_far(distance):
        return {"device_id": {"aux": partner, "row": row_of(far_layer(distance), member)}, "device_id_type": MESH}

    def t_own(j, distance):
        return pltpu.make_async_remote_copy(
            h.at[0, j, :, lanes(0)], h.at[1 + member, j, :, lanes(half)], td_s.at[j - t_from],
            hz_r.at[j, half * PARTS], **to_far(distance))

    def t_other(j, distance):
        return pltpu.make_async_remote_copy(
            t.at[j - t_from], h.at[1 + lax.rem(member + span - 1, span), j, :, lanes(half)], td_s.at[j - t_from],
            hy_r.at[j, 0, 1], **to_far(distance))

    def t_sent(j, count):
        some = h.at[pl.ds(0, 2), 0, :, pl.ds(0, count * width)]
        return pltpu.make_async_remote_copy(some, some, td_s.at[j - t_from], t_r.at[0], **to_far(0))

    def each_far(body):
        for distance in range(aux - 1, 0, -1):
            at = far_layer(distance)

            @pl.when(jnp.logical_and(transit_far == 0, jnp.logical_and(at >= 0, at < aux)))
            def _():
                body(distance)

    up, down = layer + 1 < aux, layer > 0

    barrier = pltpu.get_barrier_semaphore()
    for bit in bits:
        pl.semaphore_signal(barrier, 1, **to_aux(jnp.bitwise_xor(p, bit)))
    pl.semaphore_signal(barrier, 1, **to_row(last_member))
    for step in range(1, aux):
        pl.semaphore_signal(barrier, 1, **to_row(row_of(lax.rem(layer + step, aux), member)))

    @pl.when(main_far > 0)
    def _():
        pl.semaphore_signal(
            barrier, 1, device_id={"aux": partner, "row": row_of(p, member)}, device_id_type=MESH)

    n_far = jnp.where(transit_far == 0, jnp.where(partner < half, aux - 1 - partner, partner), 0)

    def own_c(j):
        return pltpu.make_async_copy(
            c_hbm.at[pl.ds(pl.multiple_of(p * share, share), share), pl.ds(pl.multiple_of(j * width, width), width)],
            c_piece(j, layer, member), local_c.at[j])

    for j in range(chunks):
        own_c(j).start()
    load_b = pltpu.make_async_copy(b_hbm, b, local_b)
    load_b.start()
    pl.semaphore_wait(barrier, len(bits) + aux + n_far)

    def loop_from(first, last, body):
        def step(i, carry):
            body(i)
            return carry
        lax.fori_loop(first, last, step, 0)

    def loop(count, body):
        loop_from(0, count, body)

    def pass_c(j, at_layer, spread):
        c_member(j, at_layer, 0).start()
        if spread:
            for bit in bits:
                c_aux_piece(j, at_layer, bit).start()

    def first_c():
        own_c(0).wait()
        for step in range(1, aux):
            @pl.when(layer + step < aux)
            def _():
                c_direct(layer + step).start()

            @pl.when(layer - step >= 0)
            def _():
                c_direct(layer - step).start()

        pass_c(0, layer, True)

    def start_c(j, spread=False):
        own_c(j).wait()

        @pl.when(up)
        def _():
            c_line(j, layer, 1).start()

        @pl.when(down)
        def _():
            c_line(j, layer, 0).start()

        pass_c(j, layer, spread)

    def take_first_c():
        for step in range(1, aux):
            for at_layer in (layer - step, layer + step):
                @pl.when(jnp.logical_and(at_layer >= 0, at_layer < aux))
                def _():
                    c_line(0, at_layer, 0).wait_recv()
                    pass_c(0, at_layer, True)

    def relay_c(j, spread=False):
        for step in range(1, aux):

            @pl.when(layer - step >= 0)
            def _():
                c_line(j, layer - step, 1).wait_recv()

                @pl.when(up)
                def _():
                    c_line(j, layer - step, 1).start()

                pass_c(j, layer - step, spread)

            @pl.when(layer + step < aux)
            def _():
                c_line(j, layer + step, 0).wait_recv()

                @pl.when(down)
                def _():
                    c_line(j, layer + step, 0).start()

                pass_c(j, layer + step, spread)

    def spread_c(j, spread=False):
        if not spread:
            for bit in bits:
                c_aux_members(j, 0, 0, bit).start()
        for step in range(span - 1):
            c_members(j, step).wait_recv()
            if step + 1 < span - 1:
                for at_layer in range(aux):
                    c_member(j, at_layer, step + 1).start()
            for bit in bits:
                c_aux_members(j, step + 1, 0, bit).start()

    def finish_c(j, others):
        for k in sorted(range(1, aux), key=lambda k: -(k & -k)):
            c_aux_all(j, others, k ^ (k & -k), k & -k).wait_recv()
            for bit in lower(k):
                for step in range(1, span) if others else (0,):
                    c_aux_members(j, step, k, bit).start()

    def transform(j, piece):
        def block(at_layer, at_member):
            columns = pl.ds(pl.multiple_of(row_of(at_layer, at_member) * n_rows, n_rows), n_rows)
            h_acc[...] += jnp.dot(b[:, columns], c[j, at_layer, at_member], preferred_element_type=jnp.float32)

        middle = pieces // 2

        @pl.when(piece == 0)
        def _():
            finish_c(j, 0)
            h_acc[...] = jnp.zeros_like(h_acc)

        @pl.when(piece < middle)
        def _():
            loop_from(lax.div(piece * aux, middle), lax.div((piece + 1) * aux, middle), lambda i: block(i, member))

        @pl.when(piece == middle)
        def _():
            finish_c(j, 1)

        @pl.when(piece >= middle)
        def _():
            count = aux * (span - 1)
            loop_from(
                lax.div((piece - middle) * count, middle), lax.div((piece - middle + 1) * count, middle),
                lambda i: block(lax.rem(i, aux), lax.rem(member + 1 + lax.div(i, aux), span)))

        @pl.when(piece == pieces - 1)
        def _():
            h[0, j, :, lanes(0)] = h_acc[...].astype(h.dtype)
            for bit in bits:
                h_aux(j, 0, bit).start()

            if not isinstance(j, int) or j >= t_from:
                @pl.when(jnp.logical_and(j >= t_from, transit_far == 0))
                def _():
                    t_member(j).start()
                    each_far(lambda distance: t_own(j, distance).start())

            @pl.when(j > 1)
            def _():
                send_rest(j - 1)

            send_first(j)

            if isinstance(j, int):
                spread_c(1)

            @pl.when(j + 2 < chunks)
            def _():
                spread_c(j + 2)

    def pass_member(j, i):
        @pl.when(jnp.logical_not(jnp.logical_and(main_far > 0, by_transit(j, i))))
        def _():
            h_member(j, i, 0).start()

    def pass_line(j, i, way):
        @pl.when(jnp.logical_and(up if way else down, jnp.logical_not(jnp.logical_and(is_far_way(way), by_transit(j, i)))))
        def _():
            h_line(j, i, way).start()

    def send_h(j, k):
        @pl.when(owner)
        def _():
            def send(i):
                pass_line(j, i, 1)
                pass_line(j, i, 0)
                pass_member(j, i)

            loop_from(k * PARTS, (k + 1) * PARTS, send)

    def take_h(j, k):
        h_aux(j, k ^ (k & -k), k & -k).wait_recv()
        for bit in lower(k):
            h_aux(j, k, bit).start()
        send_h(j, k)

    def send_first(j):
        send_h(j, 0)
        for k in range(1, aux // 2):
            take_h(j, k)

    def send_rest(j):
        for k in range(aux // 2, aux):
            take_h(j, k)

    def relay_h(j, i):
        for way in (1, 0):
            beyond = layer > p if way else layer < p

            @pl.when(jnp.logical_and(beyond, jnp.logical_not(jnp.logical_and(is_far_way(way), by_transit(j, i)))))
            def _():
                h_line(j, i, way).wait_recv()
                pass_line(j, i, way)
                pass_member(j, i)

    def relay_t(j):
        @pl.when(transit_far == 0)
        def _():
            t_member(j).wait_recv()
            each_far(lambda distance: t_other(j, distance).start())

    def take_own(j):
        @pl.when(jnp.logical_and(main_far > 0, j >= t_from))
        def _():
            t_own(jnp.maximum(j, t_from), 0).wait_recv()

    tile = min(TILE, n_rows)
    tiles = n_rows // tile
    all_tiles = span * tiles

    def take_members(j, half):
        for step in range(span - 1):
            h_members(j, half, step).wait_recv()
            if step + 1 < span - 1:
                loop_from(half * pieces, (half + 1) * pieces, lambda i: h_member(j, i, step + 1).start())

    def add_tile(j, n, first, last):
        line = lax.div(n, tiles)
        slot = jnp.where(line == member, own_slot, 1 + line)
        at = pl.ds(pl.multiple_of(lax.rem(n, tiles) * tile, tile), tile)
        some = pl.ds(first * width, (last - first) * width)
        k_acc[:, pl.ds(pl.multiple_of(n * tile, tile), tile)] += lax.dot_general(
            h[0, j, :, some], h[slot, j, at, some], (((1,), (1,)), ((), ())), preferred_element_type=jnp.float32)

    def update(j, piece, count, halves):
        @pl.when(piece == 0)
        def _():
            for half in halves:
                take_members(j, half)
            if 1 in halves:
                take_own(j)

        loop_from(lax.div(piece * all_tiles, count), lax.div((piece + 1) * all_tiles, count),
                  lambda n: add_tile(j, n, halves[0] * (aux // 2), (halves[-1] + 1) * (aux // 2)))

    def last_update(j):
        def own(n):
            add_tile(j, member * tiles + n, aux // 2, aux)

        def other(n):
            add_tile(j, lax.rem(member * tiles + n, all_tiles), aux // 2, aux)

        take_own(j)
        loop(tiles, own)
        take_members(j, 1)
        loop_from(tiles, all_tiles, other)

    first_c()

    def clear(n):
        columns = pl.ds(pl.multiple_of(n * tile, tile), tile)
        k_acc[:, columns] = jnp.zeros((n_rows, tile), jnp.float32)

    loop(span * tiles, clear)

    start_c(1)
    take_first_c()
    start_c(2)
    relay_c(1)
    spread_c(0, True)
    start_c(3)
    relay_c(2)
    loop_from(4, chunks, start_c)
    load_b.wait()
    loop(pieces // 2, lambda piece: transform(0, piece))
    relay_c(3)
    loop_from(pieces // 2, pieces, lambda piece: transform(0, piece))
    loop_from(4, chunks, relay_c)

    quarter = slots // 4

    def main(j):
        def slot(i):
            relay_h(j, i)
            opening = jnp.logical_and(j == 0, i < START + pieces)
            tail = jnp.logical_and(j == 1, i < START + 2 * pieces - slots)
            second = jnp.logical_or(tail, jnp.logical_and(j == 0, i >= START + pieces))
            chunk = jnp.where(opening, 1, jnp.where(second, 2, j + 2))
            from_zero = j * slots + i - START
            piece = jnp.where(opening, from_zero, jnp.where(second, from_zero - pieces, i - LATER))

            @pl.when(jnp.logical_and(j + 1 >= t_from, jnp.logical_and(i == pieces, j + 1 < chunks)))
            def _():
                relay_t(j + 1)

            @pl.when(jnp.logical_and(j == 0, i == REST))
            def _():
                send_rest(0)

            now = jnp.logical_and(jnp.logical_and(piece >= 0, piece < pieces), chunk < chunks)

            @pl.when(now)
            def _():
                transform(chunk, piece)

            @pl.when(jnp.logical_and(
                jnp.logical_and(j > 0, j < chunks - 2), jnp.logical_and(i >= quarter, i < 2 * quarter)))
            def _():
                update(j - 1, i - quarter, quarter, (0, 1))

            @pl.when(jnp.logical_and(j >= chunks - 2, i >= pieces))
            def _():
                update(j - 1, i - pieces, pieces, (0, 1))

        loop(slots, slot)

        @pl.when(j == max(chunks - 2, 0))
        def _():
            send_rest(chunks - 1)

    loop(chunks, main)
    update(chunks - 1, 0, 1, (0,))
    last_update(chunks - 1)

    for at in range(aux):
        @pl.when(layer == at)
        def _():
            if at + 1 < aux:
                c_line_sent(1, at + 1).wait_send()
            if at > 0:
                c_line_sent(0, aux - at).wait_send()
    c_direct_sent().wait_send()
    c_aux_sent().wait_send()
    h_aux_sent().wait_send()
    for step in range(span - 1):
        c_members_sent(step).wait_send()
        h_member_sent(step, 0, aux).wait_send()
        fewer = jnp.logical_and(main_far > 0, step == 0)

        @pl.when(fewer)
        def _():
            h_member_sent(step, 1, aux - 1).wait_send()

        @pl.when(jnp.logical_not(fewer))
        def _():
            h_member_sent(step, 1, aux).wait_send()

    for way, has_next, sends in ((1, up, layer >= p), (0, down, layer <= p)):
        @pl.when(jnp.logical_and(has_next, sends))
        def _():
            h_line_sent(way, 0, aux).wait_send()

            @pl.when(is_far_way(way))
            def _():
                h_line_sent(way, 1, aux - 1).wait_send()

            @pl.when(jnp.logical_not(is_far_way(way)))
            def _():
                h_line_sent(way, 1, aux).wait_send()

    @pl.when(transit_far == 0)
    def _():
        t_member_sent().wait_send()

    for index in range(aux):
        @pl.when(jnp.logical_and(transit_far == 0, partner == index))
        def _():
            count = aux - 1 - index if index < half else index
            loop_from(t_from, chunks, lambda j: t_sent(j, count).wait_send())


def body(aux, rows_axis, integrals, orbitals):
    _, n_rows, n = integrals.shape
    occ = orbitals.shape[1]
    span = rows_axis // aux
    width = CHUNK
    chunks = occ // width
    dma = pltpu.SemaphoreType.DMA
    tiles = span * (n_rows // min(TILE, n_rows))
    steps = max(span - 1, 1)
    return pl.pallas_call(
        functools.partial(kernel, aux, rows_axis),
        out_shape=pltpu.VMEM((n_rows, span * n_rows), jnp.float32),
        in_specs=[pl.BlockSpec(memory_space=pl.ANY)] * 2,
        out_specs=pl.BlockSpec(memory_space=pltpu.VMEM),
        scratch_shapes=[
            pltpu.VMEM((n_rows, n), integrals.dtype),
            pltpu.VMEM((chunks, aux, span, n_rows, width), orbitals.dtype),
            pltpu.VMEM((1 + span, chunks, n_rows, aux * width), jnp.bfloat16),
            pltpu.VMEM((chunks - TRANSIT_FROM, n_rows, width), jnp.bfloat16),
            pltpu.VMEM((n_rows, width), jnp.float32),
            dma, dma((chunks,)),
            dma((3,)), dma((chunks, aux)),
            dma((steps,)), dma((chunks, steps)),
            dma, dma((chunks, 2, aux)),
            dma, dma((chunks, aux)),
            dma((2, 2)), dma((chunks, aux * PARTS)),
            dma((steps, 2)), dma((chunks, steps, 2)),
            dma((chunks - TRANSIT_FROM,)), dma, dma((chunks - TRANSIT_FROM,)),
        ],
        compiler_params=pltpu.CompilerParams(
            collective_id=0, has_side_effects=True, vmem_limit_bytes=54 * 2**20),
    )(integrals.reshape(n_rows, n), orbitals)


def solution(mesh):
    aux, rows_axis = mesh.shape["aux"], mesh.shape["row"]
    return jax.shard_map(
        functools.partial(body, aux, rows_axis), mesh=mesh,
        in_specs=(P("aux", "row", None), P("row", None)), out_specs=P("row", "aux"), check_vma=False)
```
